512 devices in a mesh: rep: 2 (over y), gx: 128 (over x, z), gy: 2 (over core).
Axes of the slice: x: 4, y: 2, z: 32, core: 2. Of those that a mesh axis runs over, the one named last changes fastest.
The devices are a block of a 4x8x32 slice.
Arguments:
- tokens: bfloat16 [768, 8192], P(('rep', 'gx'), 'gy'), parts along dimension 0, may hold values from -6 to 6
- segment_ids: int32 [768], P(('rep', 'gx')), parts along dimension 0, may hold values from 0 to 1, as said below
- gate_weight: bfloat16 [8192, 2, 13312], P(None, 'gy', 'gx'), may hold values from -0.0625 to 0.0625
- up_weight: bfloat16 [8192, 2, 13312], P(None, 'gy', 'gx'), may hold values from -0.0625 to 0.0625
- down_weight: bfloat16 [2, 13312, 8192], P('gy', None, 'gx'), may hold values from -0.0390625 to 0.0390625
Outputs:
- grouped: bfloat16 [768, 8192], P(('rep', 'gx'), 'gy'), parts along dimension 0
The draws below stay inside these ranges and needn't reach their ends.
There are 2 independent parts, one for each index of `rep`. The reference program is written for one: setup_inputs(seed, part) draws one part's arguments, and reference() takes and returns one part's arrays. A program takes and returns all parts, laid end to end along the dimension named above; an argument that names none is the same for every part. Nothing has to cross between parts.
Inputs may be any that keep to these rules, and one draw needn't show every extreme that they name: `segment_ids`: exactly 320 entries are 0 and 64 entries are 1.
All inputs are finite; a program needn't handle non-finite values.
Results may differ from the reference program's by a relative error of at most 0.0049.
Values may be sent and summed in bfloat16 or wider, within the bound.
No kernel may reach another device: no remote copies, remote signals or barrier semaphores. Data moves between devices by JAX's collectives and lax.ppermute only.
A program may use at most 128 MiB of HBM per device.

```python
import jax
import jax.numpy as jnp

D = 8192
FF = 26624
PREFILL = 320
DECODE = 64
TOKENS = 384


def draw_segment_ids(key, part):
    shuffled = jax.random.permutation(key, PREFILL + DECODE)
    return (shuffled >= PREFILL).astype(jnp.int32)


def steps_of(own_key, shape, pieces, low, top_value):
    loudness = 1.0
    for axis_at, shards_of in pieces:
        draws = jax.random.uniform(jax.random.fold_in(jax.random.fold_in(own_key, 6), axis_at), (shards_of,), jnp.float32, low / len(pieces), top_value / len(pieces))
        loudness = loudness * jnp.repeat(jnp.exp(draws), shape[axis_at] // shards_of).reshape((-1,) + (1,) * (len(shape) - 1 - axis_at))
    return loudness


def noise(rng, shape, spread, bound, cuts=(), dtype=jnp.bfloat16):
    result = spread * jax.random.normal(rng, shape, jnp.float32)
    if cuts:
        result = result * steps_of(rng, shape, cuts, -0.22, 0.18)
    return jnp.clip(result, -bound, bound).astype(dtype)


def setup_inputs(seed: int = 0, part: int = 0) -> dict:
    key_list = jax.random.split(jax.random.key(seed), 6)
    own_keys = jax.random.split(jax.random.fold_in(key_list[5], part), 6)
    return {
        "tokens": noise(own_keys[0], (TOKENS, D), 1.0, 6.0, ((0, 128), (1, 2))),
        "segment_ids": draw_segment_ids(jax.random.fold_in(jax.random.fold_in(key_list[5], part), 71), part),
        "gate_weight": noise(key_list[2], (D, 2, FF // 2), D ** -0.5, 0.0625, ((1, 2), (2, 128))),
        "up_weight": noise(key_list[3], (D, 2, FF // 2), D ** -0.5, 0.0625, ((1, 2), (2, 128))),
        "down_weight": noise(key_list[4], (2, FF // 2, D), FF ** -0.5, 0.0390625, ((0, 2), (2, 128))),
    }


def grouped_target(segment_ids):
    decode_flag = segment_ids.astype(jnp.int32)
    prefill_flag = 1 - decode_flag
    prefill_rank = (jnp.cumsum(prefill_flag) - 1).astype(jnp.int32)
    decode_rank = (jnp.cumsum(decode_flag) - 1).astype(jnp.int32)
    return jnp.where(decode_flag == 0, prefill_rank, PREFILL + decode_rank).astype(jnp.int32)


def reference(tokens, segment_ids, gate_weight, up_weight, down_weight):
    gate_matrix = gate_weight.reshape(D, FF)
    up_matrix = up_weight.reshape(D, FF)
    down_matrix = down_weight.reshape(FF, D)
    gate_value = jnp.dot(tokens, gate_matrix, preferred_element_type=jnp.float32)
    up_value = jnp.dot(tokens, up_matrix, preferred_element_type=jnp.float32)
    hidden = (jax.nn.silu(gate_value) * up_value).astype(jnp.bfloat16)
    product = jnp.dot(hidden, down_matrix, preferred_element_type=jnp.float32)
    target = grouped_target(segment_ids)
    placed = jnp.zeros_like(product).at[target].set(product)
    return placed.astype(jnp.bfloat16)
```

```python
import functools

import jax
import jax.numpy as jnp
from jax import lax
from jax.experimental import pallas as pl
from jax.sharding import Mesh
from jax.sharding import PartitionSpec as P

PREFILL = 320
X, ZO, ZI = 4, 8, 4
GX = ("x", "zo", "zi")
REP_GX = ("rep", "x", "zo", "zi")
LANES = 128
STEPS = (0, 1, 3, 2)
F32 = jnp.float32
BF16 = jnp.bfloat16


def shifted(value, axis, by):
    count = lax.axis_size(axis)
    return lax.ppermute(value, axis, [(i, (i + by) % count) for i in range(count)])


def exchanged(blocks, axes):
    return lax.all_to_all(blocks, axes, split_axis=0, concat_axis=0, tiled=True)


def cut_kernel(depth, rows_ref, out_ref):
    for zi in range(ZI):
        pieces = [
            rows_ref[:, (zo * ZI + zi) * depth : (zo * ZI + zi + 1) * depth] for zo in range(ZO)
        ]
        out_ref[0, zi] = jnp.concatenate(pieces, axis=1)


def cut_rows(down):
    features, rows = down.shape
    depth = rows // (X * ZO * ZI)
    return pl.pallas_call(
        functools.partial(cut_kernel, depth),
        grid=(X,),
        in_specs=[pl.BlockSpec((features, rows // X), lambda i: (0, i))],
        out_specs=pl.BlockSpec((1, ZI, features, ZO * depth), lambda i: (i, 0, 0, 0)),
        out_shape=jax.ShapeDtypeStruct((X, ZI, features, ZO * depth), down.dtype),
        name="cut_rows",
    )(down)


def place_kernel(kinds_ref, order_ref, order_row_ref, slot_ref, place_ref):
    kinds = kinds_ref[...].astype(F32)
    order = order_ref[...]
    earlier = (order_row_ref[...] < order[:, :1]).astype(BF16)
    decode_before = jnp.dot(earlier, kinds.astype(BF16), preferred_element_type=F32)
    target = jnp.where(kinds > 0.5, PREFILL + decode_before, order - decode_before)
    place_ref[...] = (target[:, :1] == slot_ref[...]).astype(BF16)


def placement(kinds, x, own_tokens):
    count = kinds.shape[0]
    chunk = count // X
    k = jnp.arange(count) // chunk
    steps = jnp.array(STEPS, jnp.int32)[k]
    order = (((x - steps) % X) * chunk + jnp.arange(count) % chunk).astype(F32)
    slot = jnp.arange(count).reshape(X, ZO, ZI, own_tokens).transpose(0, 2, 1, 3).reshape(1, count)
    return pl.pallas_call(
        place_kernel,
        out_shape=jax.ShapeDtypeStruct((count, count), BF16),
        name="placement",
    )(kinds, jnp.broadcast_to(order[:, None], (count, LANES)), order[None], slot.astype(F32))


def hidden_kernel(own_ref, other_ref, place_ref, out_ref):
    value = own_ref[...] + other_ref[...]
    width = value.shape[1] // 2
    gate_value, up_value = value[:, :width], value[:, width:]
    hidden = gate_value / (1 + jnp.exp(-gate_value)) * up_value
    placed = jnp.dot(hidden.T.astype(BF16), place_ref[...], preferred_element_type=F32)
    out_ref[...] = placed.astype(BF16)


def placed_hidden(own_value, other_value, place):
    width = own_value.shape[1] // 2
    return pl.pallas_call(
        hidden_kernel,
        out_shape=jax.ShapeDtypeStruct((width, place.shape[1]), BF16),
        name="placed_hidden",
    )(own_value, other_value, place)


def local(tokens, segment_ids, gate_weight, up_weight, down_weight):
    x, gy = lax.axis_index("x"), lax.axis_index("gy")
    own_tokens, half = tokens.shape
    group = exchanged(cut_rows(down_weight[0].T).reshape(X * ZI, down_weight.shape[2], -1), ("x", "zi"))

    kinds = jnp.broadcast_to(segment_ids.astype(tokens.dtype)[:, None], (own_tokens, LANES))
    wide = jnp.concatenate([tokens, kinds], 1)
    column = lax.all_gather(wide, ("zo", "zi"), axis=0, tiled=True)
    chunks = [column] + [shifted(column, "x", by) for by in STEPS[1:]]

    gate, up = gate_weight[:, 0].T, up_weight[:, 0].T

    def rows_of(which):
        at = which * half
        return jnp.concatenate([lax.dynamic_slice_in_dim(w, at, half, 1) for w in (gate, up)], 0)

    own_rows = rows_of(gy)
    other_rows = shifted(rows_of(1 - gy), "gy", 1)

    def values(rows):
        return jnp.concatenate(
            [
                lax.dot_general(chunk[:, :half], rows, (((1,), (1,)), ((), ())), preferred_element_type=F32)
                for chunk in chunks
            ],
            0,
        )

    other_value = shifted(values(other_rows), "gy", 1)
    own_value = values(own_rows)
    place = placement(jnp.concatenate([chunk[:, half:] for chunk in chunks], 0), x, own_tokens)
    placed = placed_hidden(own_value, other_value, place)

    gathered = lax.all_gather(placed, "zo", axis=0, tiled=True)
    features = group.shape[0] * group.shape[1]
    partial = lax.dot_general(
        gathered, group.reshape(features, -1), (((0,), (1,)), ((), ())), preferred_element_type=F32
    )
    slots = partial.shape[0]
    own_half, other_half = (
        lax.dynamic_slice_in_dim(partial, k * (features // 2), features // 2, 1) for k in (gy, 1 - gy)
    )
    summed = (own_half + shifted(other_half, "gy", 1)).astype(BF16)
    arrived = exchanged(summed.reshape(X * ZI, slots // (X * ZI), -1), ("x", "zi"))
    reduced = jnp.sum(arrived.astype(F32), axis=0).astype(BF16)
    owned = exchanged(reduced.reshape(ZO, own_tokens, -1), "zo")
    owned = owned.reshape(ZO, own_tokens, X // 2, -1).transpose(1, 2, 0, 3)
    return owned.reshape(own_tokens, half)


def solution(mesh):
    torus = Mesh(
        mesh.devices.reshape(mesh.shape["rep"], X, ZO, ZI, mesh.shape["gy"]),
        ("rep", "x", "zo", "zi", "gy"),
    )
    placed = (P(REP_GX, "gy"), P(REP_GX), P(None, "gy", GX), P(None, "gy", GX), P("gy", None, GX))
    return jax.shard_map(
        local, mesh=torus, in_specs=placed, out_specs=P(REP_GX, "gy"), check_vma=False
    )
```

```python
import functools

import jax
import jax.numpy as jnp
from jax import lax
from jax.experimental import pallas as pl
from jax.experimental.pallas import tpu as pltpu
from jax.sharding import Mesh
from jax.sharding import PartitionSpec as P


PREFILL = 320
X, ZO, ZI = 4, 8, 4
GX = ("x", "zo", "zi")
REP_GX = ("rep", "x", "zo", "zi")
LANES = 128
STEPS = (0, 1, 3, 2)
F32 = jnp.float32
BF16 = jnp.bfloat16


def shifted(value, axis, by):
    count = lax.axis_size(axis)
    return lax.ppermute(value, axis, [(i, (i + by) % count) for i in range(count)])


def exchanged(blocks, axes):
    return lax.all_to_all(blocks, axes, split_axis=0, concat_axis=0, tiled=True)


def copy_kernel(rows_ref, out_ref):
    out_ref[0] = rows_ref[...]


def cut_by_x(down):
    features, rows = down.shape
    return pl.pallas_call(
        copy_kernel,
        grid=(X,),
        in_specs=[pl.BlockSpec((features, rows // X), lambda i: (0, i))],
        out_specs=pl.BlockSpec((1, features, rows // X), lambda i: (i, 0, 0)),
        out_shape=jax.ShapeDtypeStruct((X, features, rows // X), down.dtype),
        name="cut_by_x",
    )(down)


def cut_kernel(depth, gy_ref, rows_ref, out_ref):
    for zi in range(ZI):
        pieces = [rows_ref[0, :, (zo * ZI + zi) * depth : (zo * ZI + zi + 1) * depth] for zo in range(ZO)]
        out_ref[zi, 0] = jnp.concatenate(pieces, axis=1)


def cut_by_zi(blocks, gy):
    count, features, rows = blocks.shape
    depth = rows // (ZO * ZI)
    return pl.pallas_call(
        functools.partial(cut_kernel, depth),
        grid_spec=pltpu.PrefetchScalarGridSpec(
            num_scalar_prefetch=1,
            grid=(count,),
            in_specs=[
                pl.BlockSpec((1, features, rows), lambda i, gy: (lax.rem(i + gy[0] * (X // 2), X), 0, 0))
            ],
            out_specs=pl.BlockSpec((ZI, 1, features, ZO * depth), lambda i, gy: (0, i, 0, 0)),
        ),
        out_shape=jax.ShapeDtypeStruct((ZI, count, features, ZO * depth), blocks.dtype),
        name="cut_by_zi",
    )(gy, blocks)


def values_kernel(chunk_ref, own_rows_ref, other_rows_ref, own_ref, other_ref):
    chunk = chunk_ref[...]
    for rows, out in ((other_rows_ref, other_ref), (own_rows_ref, own_ref)):
        out[...] = lax.dot_general(chunk, rows[...], (((1,), (1,)), ((), ())), preferred_element_type=F32)


def values(chunk, own_rows, other_rows):
    count, (columns, half) = chunk.shape[0], own_rows.shape
    out = jax.ShapeDtypeStruct((count, columns), F32)
    whole = pl.BlockSpec((columns, half), lambda i: (0, 0))
    out_spec = pl.BlockSpec((count, columns), lambda i: (0, 0))
    return pl.pallas_call(
        values_kernel,
        grid=(1,),
        in_specs=[pl.BlockSpec((count, half), lambda i: (0, 0)), whole, whole],
        out_specs=[out_spec, out_spec],
        out_shape=[out, out],
        name="values",
    )(chunk, own_rows, other_rows)


def place_kernel(*refs):
    *kinds_refs, order_ref, order_row_ref, slot_ref, place_ref = refs
    kinds = jnp.concatenate([ref[...] for ref in kinds_refs], 0)
    order = order_ref[...]
    earlier = (order_row_ref[...] < order[:, :1]).astype(BF16)
    decode_before = jnp.dot(earlier, kinds, preferred_element_type=F32)
    target = jnp.where(kinds.astype(F32) > 0.5, PREFILL + decode_before, order - decode_before)
    place_ref[...] = (target[:, :1] == slot_ref[...]).astype(BF16)


def token_order(x, chunk):
    count = X * chunk
    steps = jnp.array(STEPS, jnp.int32)[jnp.arange(count) // chunk]
    order = (((x - steps) % X) * chunk + jnp.arange(count) % chunk).astype(F32)
    return jnp.broadcast_to(order[:, None], (count, LANES)), order[None]


def placement(chunks, half, order, order_row, own_tokens):
    chunk = chunks[0].shape[0]
    count = X * chunk
    slot = jnp.arange(count).reshape(X, ZO, ZI, own_tokens).transpose(0, 2, 1, 3).reshape(1, count)
    kinds = pl.BlockSpec((chunk, LANES), lambda i: (0, half // LANES))
    one_row = pl.BlockSpec((1, count), lambda i: (0, 0))
    return pl.pallas_call(
        place_kernel,
        grid=(1,),
        in_specs=[kinds] * X + [pl.BlockSpec((count, LANES), lambda i: (0, 0)), one_row, one_row],
        out_specs=pl.BlockSpec((count, count), lambda i: (0, 0)),
        out_shape=jax.ShapeDtypeStruct((count, count), BF16),
        name="placement",
    )(*chunks, order, order_row, slot.astype(F32))


def hidden_kernel(*refs):
    *own_refs, other_ref, place_ref, out_ref = refs
    value = jnp.concatenate([ref[...] for ref in own_refs], 0) + other_ref[...]
    width = value.shape[1] // 2
    gate_value, up_value = value[:, :width], value[:, width:]
    hidden = gate_value / (1 + jnp.exp(-gate_value)) * up_value
    placed = jnp.dot(hidden.T.astype(BF16), place_ref[...], preferred_element_type=F32)
    out_ref[...] = placed.astype(BF16)


def placed_hidden(own_values, other_value, place):
    width = other_value.shape[1] // 2
    return pl.pallas_call(
        hidden_kernel,
        out_shape=jax.ShapeDtypeStruct((width, place.shape[1]), BF16),
        name="placed_hidden",
    )(*own_values, other_value, place)


def block(tokens, segment_ids, gate_weight, up_weight, down_weight):
    x, gy = lax.axis_index("x"), lax.axis_index("gy")
    own_tokens, half = tokens.shape
    down = exchanged(cut_by_x(down_weight[0].T), "x")

    kinds = jnp.broadcast_to(segment_ids.astype(tokens.dtype)[:, None], (own_tokens, LANES))
    wide = jnp.concatenate([tokens, kinds], 1)
    order, order_row = token_order(x, own_tokens * ZO * ZI)
    column = lax.all_gather(wide, ("zo", "zi"), axis=0, tiled=True)
    column, gate, up = lax.optimization_barrier((column, gate_weight, up_weight))
    gate, up = gate[:, 0].T, up[:, 0].T
    chunks = [column]
    for by in STEPS[1:]:
        chunks.append(shifted(column, "x", by))

    group = cut_by_zi(down, gy.reshape(1))
    group = exchanged(group, "zi")

    def rows_of(which):
        at = which * half
        return jnp.concatenate([lax.dynamic_slice_in_dim(w, at, half, 1) for w in (gate, up)], 0)

    own_rows = rows_of(gy)
    other_rows = shifted(rows_of(1 - gy), "gy", 1)

    own_values, other_values = [], []
    for by, chunk in zip(STEPS, chunks, strict=True):
        own_value, other_value = values(chunk, own_rows, other_rows)
        own_values.append(own_value)
        other_values.append(other_value)
    other_value = shifted(jnp.concatenate(other_values, 0), "gy", 1)
    place = placement(chunks, half, order, order_row, own_tokens)
    placed = placed_hidden(own_values, other_value, place)

    gathered = lax.all_gather(placed, "zo", axis=0, tiled=True)

    depth = group.shape[3]
    partial = lax.dot_general(
        gathered, group.reshape(-1, depth), (((0,), (1,)), ((), ())), preferred_element_type=F32
    )
    width = partial.shape[1] // (2 * ZI)

    def half_of(which):
        return jnp.concatenate(
            [partial[:, (2 * k + which) * width : (2 * k + which + 1) * width] for k in range(ZI)], 1
        )

    other_half = shifted(half_of(1), "gy", 1)
    summed = (half_of(0) + other_half).astype(BF16)
    slots = summed.shape[0]
    arrived = exchanged(summed.reshape(X * ZI, slots // (X * ZI), -1), ("x", "zi"))
    reduced = jnp.sum(arrived.astype(F32), axis=0).astype(BF16)
    owned = exchanged(reduced.reshape(ZO, own_tokens, -1), "zo")
    owned = owned.reshape(ZO, own_tokens, ZI, X // 2, -1).transpose(1, 3, 0, 2, 4)
    return owned.reshape(own_tokens, half)


def solution(mesh):
    torus = Mesh(
        mesh.devices.reshape(mesh.shape["rep"], X, ZO, ZI, mesh.shape["gy"]),
        ("rep", "x", "zo", "zi", "gy"),
    )
    placed = (P(REP_GX, "gy"), P(REP_GX), P(None, "gy", GX), P(None, "gy", GX), P("gy", None, GX))
    return jax.shard_map(block, mesh=torus, in_specs=placed, out_specs=P(REP_GX, "gy"), check_vma=False)
```

```python
import functools

import jax
import jax.numpy as jnp
import numpy as np
from jax import lax
from jax.experimental import pallas as pl
from jax.experimental.pallas import tpu as pltpu
from jax.sharding import Mesh
from jax.sharding import PartitionSpec as P


PREFILL = 320
X, ZO, ZI = 4, 8, 4
GX = ("x", "zo", "zi")
REP_GX = ("rep", "x", "zo", "zi")
LANES = 128
STEPS = (0, 1, 3, 2)
F32 = jnp.float32
BF16 = jnp.bfloat16


def shifted(value, axis, by):
    count = lax.axis_size(axis)
    return lax.ppermute(value, axis, [(i, (i + by) % count) for i in range(count)])


def exchanged(blocks, axes):
    return lax.all_to_all(blocks, axes, split_axis=0, concat_axis=0, tiled=True)


HBM = pl.BlockSpec(memory_space=pl.ANY)


def run_copies(copies):
    for copy in copies:
        copy.start()
    for copy in copies:
        copy.wait()


def cut_by_x_kernel(rows_ref, out_ref, sems):
    rows = out_ref.shape[2]
    run_copies(
        [
            pltpu.make_async_copy(rows_ref.at[:, pl.ds(k * rows, rows)], out_ref.at[k], sems.at[k])
            for k in range(X)
        ]
    )


def cut_by_x(down):
    features, rows = down.shape
    return pl.pallas_call(
        cut_by_x_kernel,
        in_specs=[HBM],
        out_specs=HBM,
        out_shape=jax.ShapeDtypeStruct((X, features, rows // X), down.dtype),
        scratch_shapes=[pltpu.SemaphoreType.DMA((X,))],
        name="cut_by_x",
    )(down)


def split_kernel(gy_ref, gate_ref, up_ref, own_ref, other_ref, sems):
    half = own_ref.shape[2]
    gy = gy_ref[0]
    copies = []
    for k, ref in enumerate((gate_ref, up_ref)):
        for j, (out, which) in enumerate(((other_ref, 1 - gy), (own_ref, gy))):
            columns = pl.ds(pl.multiple_of(which * half, LANES), half)
            copies.append(pltpu.make_async_copy(ref.at[:, columns], out.at[k], sems.at[2 * k + j]))
    run_copies(copies)


def split_rows(gate, up, gy):
    columns, both = gate.shape
    out = jax.ShapeDtypeStruct((2, columns, both // 2), gate.dtype)
    own, other = pl.pallas_call(
        split_kernel,
        in_specs=[pl.BlockSpec(memory_space=pltpu.SMEM), HBM, HBM],
        out_specs=[HBM, HBM],
        out_shape=[out, out],
        scratch_shapes=[pltpu.SemaphoreType.DMA((4,))],
        name="split_rows",
    )(gy, gate, up)
    return own.reshape(2 * columns, -1), other.reshape(2 * columns, -1)


def cut_kernel(depth, gy_ref, rows_ref, out_ref):
    for zi in range(ZI):
        pieces = [rows_ref[0, :, (zo * ZI + zi) * depth : (zo * ZI + zi + 1) * depth] for zo in range(ZO)]
        out_ref[zi, 0] = jnp.concatenate(pieces, axis=1)


def cut_by_zi(blocks, gy):
    count, features, rows = blocks.shape
    depth = rows // (ZO * ZI)
    return pl.pallas_call(
        functools.partial(cut_kernel, depth),
        grid_spec=pltpu.PrefetchScalarGridSpec(
            num_scalar_prefetch=1,
            grid=(count,),
            in_specs=[
                pl.BlockSpec((1, features, rows), lambda i, gy: (lax.rem(i + gy[0] * (X // 2), X), 0, 0))
            ],
            out_specs=pl.BlockSpec((ZI, 1, features, ZO * depth), lambda i, gy: (0, i, 0, 0)),
        ),
        out_shape=jax.ShapeDtypeStruct((ZI, count, features, ZO * depth), blocks.dtype),
        name="cut_by_zi",
    )(gy, blocks)


def values_kernel(*refs):
    *chunk_refs, own_rows_ref, other_rows_ref, own_ref, other_ref = refs
    step = pl.program_id(0)
    chunks = jnp.concatenate([ref[...] for ref in chunk_refs], 0)
    for rows, out in ((other_rows_ref, other_ref), (own_rows_ref, own_ref)):
        term = lax.dot_general(chunks, rows[...], (((1,), (1,)), ((), ())), preferred_element_type=F32)

        @pl.when(step == 0)
        def _():
            out[...] = term

        @pl.when(step > 0)
        def _():
            out[...] += term


def values(chunks, own_rows, other_rows, steps=4):
    count, (columns, half) = chunks[0].shape[0], own_rows.shape
    depth = half // steps
    out = jax.ShapeDtypeStruct((len(chunks) * count, columns), F32)
    rows = pl.BlockSpec((columns, depth), lambda i: (0, i))
    out_spec = pl.BlockSpec(out.shape, lambda i: (0, 0))
    return pl.pallas_call(
        values_kernel,
        grid=(steps,),
        in_specs=[pl.BlockSpec((count, depth), lambda i: (0, i))] * len(chunks) + [rows, rows],
        out_specs=[out_spec, out_spec],
        out_shape=[out, out],
        name="values",
    )(*chunks, own_rows, other_rows)


def place_kernel(x_ref, *refs):
    *kinds_refs, slot_ref, place_ref = refs
    chunk, count = kinds_refs[0].shape[0], slot_ref.shape[1]
    starts = [lax.rem(x_ref[0] + X - by, X) * chunk for by in STEPS]
    lane = lax.broadcasted_iota(jnp.int32, (1, count), 1)
    order_row = lane + starts[0]
    for k in range(1, X):
        order_row = jnp.where(lane < k * chunk, order_row, lane - k * chunk + starts[k])
    kinds = jnp.concatenate([ref[...] for ref in kinds_refs], 0)
    place = lax.broadcasted_iota(jnp.int32, (chunk, LANES), 0)
    order = jnp.concatenate([place + start for start in starts], 0)
    earlier = (order_row.astype(F32) < order[:, :1].astype(F32)).astype(BF16)
    decode_before = jnp.dot(earlier, kinds, preferred_element_type=F32)
    target = jnp.where(kinds.astype(F32) > 0.5, PREFILL + decode_before, order.astype(F32) - decode_before)
    place_ref[...] = (target[:, :1] == slot_ref[...]).astype(BF16)


def placement(chunks, half, x, own_tokens):
    chunk = chunks[0].shape[0]
    count = X * chunk
    slot = np.arange(count).reshape(X, ZO, ZI, own_tokens).transpose(0, 2, 1, 3).reshape(1, count)
    kinds = pl.BlockSpec((chunk, LANES), lambda i: (0, half // LANES))
    return pl.pallas_call(
        place_kernel,
        grid=(1,),
        in_specs=[pl.BlockSpec(memory_space=pltpu.SMEM)]
        + [kinds] * X
        + [pl.BlockSpec((1, count), lambda i: (0, 0))],
        out_specs=pl.BlockSpec((count, count), lambda i: (0, 0)),
        out_shape=jax.ShapeDtypeStruct((count, count), BF16),
        name="placement",
    )(x, *chunks, slot.astype(np.float32))


def hidden_kernel(own_ref, other_ref, place_ref, out_ref):
    value = own_ref[...] + other_ref[...]
    width = value.shape[1] // 2
    gate_value, up_value = value[:, :width], value[:, width:]
    hidden = gate_value / (1 + jnp.exp(-gate_value)) * up_value
    placed = jnp.dot(hidden.T.astype(BF16), place_ref[...], preferred_element_type=F32)
    out_ref[...] = placed.astype(BF16)


def placed_hidden(own_value, other_value, place):
    width = other_value.shape[1] // 2
    return pl.pallas_call(
        hidden_kernel,
        out_shape=jax.ShapeDtypeStruct((width, place.shape[1]), BF16),
        name="placed_hidden",
    )(own_value, other_value, place)


def block(tokens, segment_ids, gate_weight, up_weight, down_weight):
    x, gy = lax.axis_index("x"), lax.axis_index("gy")
    own_tokens, half = tokens.shape
    down = exchanged(cut_by_x(down_weight[0].T), "x")

    kinds = jnp.broadcast_to(segment_ids.astype(tokens.dtype)[:, None], (own_tokens, LANES))
    wide = jnp.concatenate([tokens, kinds], 1)
    column = lax.all_gather(wide, ("zo", "zi"), axis=0, tiled=True)
    column, gate, up = lax.optimization_barrier((column, gate_weight, up_weight))
    gate, up = gate[:, 0].T, up[:, 0].T
    chunks = [column]
    for by in STEPS[1:]:
        chunks.append(shifted(column, "x", by))

    group = cut_by_zi(down, gy.reshape(1))
    group = exchanged(group, "zi")

    own_rows, other_rows = split_rows(gate, up, gy.reshape(1))
    other_rows = shifted(other_rows, "gy", 1)

    own_value, other_value = values(chunks, own_rows, other_rows)
    other_value = shifted(other_value, "gy", 1)
    place = placement(chunks, half, x.reshape(1), own_tokens)
    placed = placed_hidden(own_value, other_value, place)

    gathered = lax.all_gather(placed, "zo", axis=0, tiled=True)

    depth = group.shape[3]
    partial = lax.dot_general(
        gathered, group.reshape(-1, depth), (((0,), (1,)), ((), ())), preferred_element_type=F32
    )
    width = partial.shape[1] // (2 * ZI)

    def half_of(which):
        return jnp.concatenate(
            [partial[:, (2 * k + which) * width : (2 * k + which + 1) * width] for k in range(ZI)], 1
        )

    other_half = shifted(half_of(1), "gy", 1)
    summed = (half_of(0) + other_half).astype(BF16)
    slots = summed.shape[0]
    arrived = exchanged(summed.reshape(X * ZI, slots // (X * ZI), -1), ("x", "zi"))
    reduced = jnp.sum(arrived.astype(F32), axis=0).astype(BF16)
    owned = exchanged(reduced.reshape(ZO, own_tokens, -1), "zo")
    owned = owned.reshape(ZO, own_tokens, ZI, X // 2, -1).transpose(1, 3, 0, 2, 4)
    return owned.reshape(own_tokens, half)


def solution(mesh):
    torus = Mesh(
        mesh.devices.reshape(mesh.shape["rep"], X, ZO, ZI, mesh.shape["gy"]),
        ("rep", "x", "zo", "zi", "gy"),
    )
    placed = (P(REP_GX, "gy"), P(REP_GX), P(None, "gy", GX), P(None, "gy", GX), P("gy", None, GX))
    return jax.shard_map(block, mesh=torus, in_specs=placed, out_specs=P(REP_GX, "gy"), check_vma=False)
```

```python
import functools

import jax
import jax.numpy as jnp
import numpy as np
from jax import lax
from jax.experimental import pallas as pl
from jax.experimental.pallas import tpu as pltpu
from jax.sharding import Mesh
from jax.sharding import PartitionSpec as P


PREFILL = 320
X, ZO, ZI = 4, 8, 4
GX = ("x", "zo", "zi")
REP_GX = ("rep", "x", "zo", "zi")
LANES = 128
STEPS = (0, 1, 3, 2)
F32 = jnp.float32
BF16 = jnp.bfloat16


def shifted(value, axis, by):
    count = lax.axis_size(axis)
    return lax.ppermute(value, axis, [(i, (i + by) % count) for i in range(count)])


def exchanged(blocks, axes):
    return lax.all_to_all(blocks, axes, split_axis=0, concat_axis=0, tiled=True)


HBM = pl.BlockSpec(memory_space=pl.ANY)


def cut_by_x_kernel(rows_ref, out_ref, held, in_sems, out_sems):
    rows = out_ref.shape[2]
    ins = [
        pltpu.make_async_copy(rows_ref.at[:, pl.ds(k * rows, rows)], held.at[k], in_sems.at[k])
        for k in range(X)
    ]
    outs = [pltpu.make_async_copy(held.at[k], out_ref.at[k], out_sems.at[k]) for k in range(X)]
    for copy in ins:
        copy.start()
    for arrive, leave in zip(ins, outs, strict=True):
        arrive.wait()
        leave.start()
    for copy in outs:
        copy.wait()


def cut_by_x(down):
    features, rows = down.shape
    shape = (X, features, rows // X)
    return pl.pallas_call(
        cut_by_x_kernel,
        in_specs=[HBM],
        out_specs=HBM,
        out_shape=jax.ShapeDtypeStruct(shape, down.dtype),
        scratch_shapes=[
            pltpu.VMEM(shape, down.dtype),
            pltpu.SemaphoreType.DMA((X,)),
            pltpu.SemaphoreType.DMA((X,)),
        ],
        name="cut_by_x",
    )(down)


def cut_kernel(depth, gy_ref, rows_ref, out_ref):
    for zi in range(ZI):
        pieces = [rows_ref[0, :, (zo * ZI + zi) * depth : (zo * ZI + zi + 1) * depth] for zo in range(ZO)]
        out_ref[zi, 0] = jnp.concatenate(pieces, axis=1)


def cut_by_zi(blocks, gy):
    count, features, rows = blocks.shape
    depth = rows // (ZO * ZI)
    return pl.pallas_call(
        functools.partial(cut_kernel, depth),
        grid_spec=pltpu.PrefetchScalarGridSpec(
            num_scalar_prefetch=1,
            grid=(count,),
            in_specs=[
                pl.BlockSpec((1, features, rows), lambda i, gy: (lax.rem(i + gy[0] * (X // 2), X), 0, 0))
            ],
            out_specs=pl.BlockSpec((ZI, 1, features, ZO * depth), lambda i, gy: (0, i, 0, 0)),
        ),
        out_shape=jax.ShapeDtypeStruct((ZI, count, features, ZO * depth), blocks.dtype),
        name="cut_by_zi",
    )(gy, blocks)


def place_kernel(x_ref, *refs):
    *kinds_refs, slot_ref, place_ref = refs
    chunk, count = kinds_refs[0].shape[0], slot_ref.shape[1]
    starts = [lax.rem(x_ref[0] + X - by, X) * chunk for by in STEPS]
    lane = lax.broadcasted_iota(jnp.int32, (1, count), 1)
    order_row = lane + starts[0]
    for k in range(1, X):
        order_row = jnp.where(lane < k * chunk, order_row, lane - k * chunk + starts[k])
    kinds = jnp.concatenate([ref[...] for ref in kinds_refs], 0)
    place = lax.broadcasted_iota(jnp.int32, (chunk, LANES), 0)
    order = jnp.concatenate([place + start for start in starts], 0)
    earlier = (order_row.astype(F32) < order[:, :1].astype(F32)).astype(BF16)
    decode_before = jnp.dot(earlier, kinds, preferred_element_type=F32)
    target = jnp.where(kinds.astype(F32) > 0.5, PREFILL + decode_before, order.astype(F32) - decode_before)
    place_ref[...] = (target[:, :1] == slot_ref[...]).astype(BF16)


def placement(chunks, half, x, own_tokens):
    chunk = chunks[0].shape[0]
    count = X * chunk
    slot = np.arange(count).reshape(X, ZO, ZI, own_tokens).transpose(0, 2, 1, 3).reshape(1, count)
    kinds = pl.BlockSpec((chunk, LANES), lambda i: (0, half // LANES))
    return pl.pallas_call(
        place_kernel,
        grid=(1,),
        in_specs=[pl.BlockSpec(memory_space=pltpu.SMEM)]
        + [kinds] * X
        + [pl.BlockSpec((1, count), lambda i: (0, 0))],
        out_specs=pl.BlockSpec((count, count), lambda i: (0, 0)),
        out_shape=jax.ShapeDtypeStruct((count, count), BF16),
        name="placement",
    )(x, *chunks, slot.astype(np.float32))


def hidden_kernel(gy_ref, *refs):
    own_refs, other_refs = refs[:X], refs[X : 2 * X]
    gate_own, gate_other, up_own, up_other, place_ref, out_ref, gate_sum, up_sum = refs[2 * X :]
    step = pl.program_id(0)
    own, other = (jnp.concatenate([ref[...] for ref in part], 0) for part in (own_refs, other_refs))
    across = (((1,), (1,)), ((), ()))
    for total, rows, other_rows in ((gate_sum, gate_own, gate_other), (up_sum, up_own, up_other)):
        term = lax.dot_general(rows[...], own, across, preferred_element_type=F32)
        term += lax.dot_general(other_rows[...], other, across, preferred_element_type=F32)

        @pl.when(step == 0)
        def _():
            total[...] = term

        @pl.when(step > 0)
        def _():
            total[...] += term

    @pl.when(step == pl.num_programs(0) - 1)
    def _():
        gate_value = gate_sum[...]
        hidden = (gate_value / (1 + jnp.exp(-gate_value)) * up_sum[...]).astype(BF16)
        out_ref[...] = jnp.dot(hidden, place_ref[...], preferred_element_type=F32).astype(BF16)


def placed_hidden(chunks, other_chunks, gate, up, place, gy, steps=4):
    columns, features = gate.shape
    half = features // 2
    depth = half // steps
    chunk, slots = chunks[0].shape[0], place.shape[1]
    tokens = pl.BlockSpec((chunk, depth), lambda i, gy: (0, i))
    own = pl.BlockSpec((columns, depth), lambda i, gy: (0, gy[0] * steps + i))
    other = pl.BlockSpec((columns, depth), lambda i, gy: (0, (1 - gy[0]) * steps + i))
    return pl.pallas_call(
        hidden_kernel,
        grid_spec=pltpu.PrefetchScalarGridSpec(
            num_scalar_prefetch=1,
            grid=(steps,),
            in_specs=[tokens] * (2 * X) + [own, other, own, other] + [pl.BlockSpec(place.shape, lambda i, gy: (0, 0))],
            out_specs=pl.BlockSpec((columns, slots), lambda i, gy: (0, 0)),
            scratch_shapes=[pltpu.VMEM((columns, slots), F32)] * 2,
        ),
        out_shape=jax.ShapeDtypeStruct((columns, slots), BF16),
        name="placed_hidden",
    )(gy, *chunks, *other_chunks, gate, gate, up, up, place)


def block(tokens, segment_ids, gate_weight, up_weight, down_weight):
    x, gy = lax.axis_index("x"), lax.axis_index("gy")
    own_tokens, half = tokens.shape
    down = exchanged(cut_by_x(down_weight[0].T), "x")

    kinds = jnp.broadcast_to(segment_ids.astype(tokens.dtype)[:, None], (own_tokens, LANES))
    wide = jnp.concatenate([tokens, kinds], 1)
    column = lax.all_gather(wide, ("zo", "zi"), axis=0, tiled=True)
    gate, up = gate_weight[:, 0].T, up_weight[:, 0].T
    chunks = [column]
    for by in STEPS[1:]:
        chunks.append(shifted(column, "x", by))
    other_chunks = []
    for by, chunk in zip(STEPS, chunks, strict=True):
        other_chunks.append(shifted(chunk, "gy", 1))

    group = cut_by_zi(down, gy.reshape(1))
    group = exchanged(group, "zi")

    place = placement(chunks, half, x.reshape(1), own_tokens)
    placed = placed_hidden(chunks, other_chunks, gate, up, place, gy.reshape(1))

    gathered = lax.all_gather(placed, "zo", axis=0, tiled=True)

    depth = group.shape[3]
    partial = lax.dot_general(
        gathered, group.reshape(-1, depth), (((0,), (1,)), ((), ())), preferred_element_type=F32
    )
    width = partial.shape[1] // (2 * ZI)

    def half_of(which):
        return jnp.concatenate(
            [partial[:, (2 * k + which) * width : (2 * k + which + 1) * width] for k in range(ZI)], 1
        )

    other_half = shifted(half_of(1), "gy", 1)
    summed = (half_of(0) + other_half).astype(BF16)
    slots = summed.shape[0]
    arrived = exchanged(summed.reshape(X * ZI, slots // (X * ZI), -1), ("x", "zi"))
    reduced = jnp.sum(arrived.astype(F32), axis=0).astype(BF16)
    owned = exchanged(reduced.reshape(ZO, own_tokens, -1), "zo")
    owned = owned.reshape(ZO, own_tokens, ZI, X // 2, -1).transpose(1, 3, 0, 2, 4)
    return owned.reshape(own_tokens, half)


def solution(mesh):
    torus = Mesh(
        mesh.devices.reshape(mesh.shape["rep"], X, ZO, ZI, mesh.shape["gy"]),
        ("rep", "x", "zo", "zi", "gy"),
    )
    placed = (P(REP_GX, "gy"), P(REP_GX), P(None, "gy", GX), P(None, "gy", GX), P("gy", None, GX))
    return jax.shard_map(block, mesh=torus, in_specs=placed, out_specs=P(REP_GX, "gy"), check_vma=False)
```

```python
import functools

import jax
import jax.numpy as jnp
import numpy as np
from jax import lax
from jax.experimental import pallas as pl
from jax.experimental.pallas import tpu as pltpu
from jax.sharding import Mesh
from jax.sharding import PartitionSpec as P


PREFILL = 320
X, ZO, ZI = 4, 8, 4
GX = ("x", "zo", "zi")
REP_GX = ("rep", "x", "zo", "zi")
LANES = 128
STEPS = (0, 1, 3, 2)
F32 = jnp.float32
BF16 = jnp.bfloat16


def shifted(value, axis, by):
    count = lax.axis_size(axis)
    return lax.ppermute(value, axis, [(i, (i + by) % count) for i in range(count)])


def exchanged(blocks, axes):
    return lax.all_to_all(blocks, axes, split_axis=0, concat_axis=0, tiled=True)


HBM = pl.BlockSpec(memory_space=pl.ANY)


def pass_on(ins, outs):
    for copy in ins:
        copy.start()
    for arrive, leave in zip(ins, outs, strict=True):
        arrive.wait()
        leave.start()
    for copy in outs:
        copy.wait()


def cut_by_x_kernel(rows_ref, out_ref, held, in_sems, out_sems):
    rows = out_ref.shape[2]
    ins = [
        pltpu.make_async_copy(rows_ref.at[:, pl.ds(k * rows, rows)], held.at[k], in_sems.at[k])
        for k in range(X)
    ]
    outs = [pltpu.make_async_copy(held.at[k], out_ref.at[k], out_sems.at[k]) for k in range(X)]
    pass_on(ins, outs)


def cut_by_x(down):
    features, rows = down.shape
    shape = (X, features, rows // X)
    return pl.pallas_call(
        cut_by_x_kernel,
        in_specs=[HBM],
        out_specs=HBM,
        out_shape=jax.ShapeDtypeStruct(shape, down.dtype),
        scratch_shapes=[
            pltpu.VMEM(shape, down.dtype),
            pltpu.SemaphoreType.DMA((X,)),
            pltpu.SemaphoreType.DMA((X,)),
        ],
        name="cut_by_x",
    )(down)


def split_kernel(gy_ref, gate_ref, up_ref, own_ref, other_ref, held, in_sems, out_sems):
    half = own_ref.shape[2]
    gy = gy_ref[0]
    ins, outs = [], []
    for k, ref in enumerate((gate_ref, up_ref)):
        for j, (out, which) in enumerate(((other_ref, 1 - gy), (own_ref, gy))):
            slot = 2 * k + j
            columns = pl.ds(pl.multiple_of(which * half, LANES), half)
            ins.append(pltpu.make_async_copy(ref.at[:, columns], held.at[slot], in_sems.at[slot]))
            outs.append(pltpu.make_async_copy(held.at[slot], out.at[k], out_sems.at[slot]))
    pass_on(ins, outs)


def split_rows(gate, up, gy):
    columns, both = gate.shape
    out = jax.ShapeDtypeStruct((2, columns, both // 2), gate.dtype)
    own, other = pl.pallas_call(
        split_kernel,
        in_specs=[pl.BlockSpec(memory_space=pltpu.SMEM), HBM, HBM],
        out_specs=[HBM, HBM],
        out_shape=[out, out],
        scratch_shapes=[
            pltpu.VMEM((4, columns, both // 2), gate.dtype),
            pltpu.SemaphoreType.DMA((4,)),
            pltpu.SemaphoreType.DMA((4,)),
        ],
        name="split_rows",
    )(gy, gate, up)
    return own.reshape(2 * columns, -1), other.reshape(2 * columns, -1)


def cut_kernel(depth, gy_ref, rows_ref, out_ref):
    for zi in range(ZI):
        pieces = [rows_ref[0, :, (zo * ZI + zi) * depth : (zo * ZI + zi + 1) * depth] for zo in range(ZO)]
        out_ref[zi, 0] = jnp.concatenate(pieces, axis=1)


def cut_by_zi(blocks, gy):
    count, features, rows = blocks.shape
    depth = rows // (ZO * ZI)
    return pl.pallas_call(
        functools.partial(cut_kernel, depth),
        grid_spec=pltpu.PrefetchScalarGridSpec(
            num_scalar_prefetch=1,
            grid=(count,),
            in_specs=[
                pl.BlockSpec((1, features, rows), lambda i, gy: (lax.rem(i + gy[0] * (X // 2), X), 0, 0))
            ],
            out_specs=pl.BlockSpec((ZI, 1, features, ZO * depth), lambda i, gy: (0, i, 0, 0)),
        ),
        out_shape=jax.ShapeDtypeStruct((ZI, count, features, ZO * depth), blocks.dtype),
        name="cut_by_zi",
    )(gy, blocks)


def place_kernel(x_ref, *refs):
    *kinds_refs, slot_ref, place_ref = refs
    chunk, count = kinds_refs[0].shape[0], slot_ref.shape[1]
    starts = [lax.rem(x_ref[0] + X - by, X) * chunk for by in STEPS]
    lane = lax.broadcasted_iota(jnp.int32, (1, count), 1)
    order_row = lane + starts[0]
    for k in range(1, X):
        order_row = jnp.where(lane < k * chunk, order_row, lane - k * chunk + starts[k])
    kinds = jnp.concatenate([ref[...] for ref in kinds_refs], 0)
    place = lax.broadcasted_iota(jnp.int32, (chunk, LANES), 0)
    order = jnp.concatenate([place + start for start in starts], 0)
    earlier = (order_row.astype(F32) < order[:, :1].astype(F32)).astype(BF16)
    decode_before = jnp.dot(earlier, kinds, preferred_element_type=F32)
    target = jnp.where(kinds.astype(F32) > 0.5, PREFILL + decode_before, order.astype(F32) - decode_before)
    place_ref[...] = (target[:, :1] == slot_ref[...]).astype(BF16)


def placement(chunks, half, x, own_tokens):
    chunk = chunks[0].shape[0]
    count = X * chunk
    slot = np.arange(count).reshape(X, ZO, ZI, own_tokens).transpose(0, 2, 1, 3).reshape(1, count)
    kinds = pl.BlockSpec((chunk, LANES), lambda i: (0, half // LANES))
    return pl.pallas_call(
        place_kernel,
        grid=(1,),
        in_specs=[pl.BlockSpec(memory_space=pltpu.SMEM)]
        + [kinds] * X
        + [pl.BlockSpec((1, count), lambda i: (0, 0))],
        out_specs=pl.BlockSpec((count, count), lambda i: (0, 0)),
        out_shape=jax.ShapeDtypeStruct((count, count), BF16),
        name="placement",
    )(x, *chunks, slot.astype(np.float32))


def values_kernel(*refs):
    *chunk_refs, own_rows_ref, other_rows_ref, own_ref, other_ref = refs
    step = pl.program_id(0)
    chunks = jnp.concatenate([ref[...] for ref in chunk_refs], 0)
    for rows, out in ((other_rows_ref, other_ref), (own_rows_ref, own_ref)):
        term = lax.dot_general(rows[...], chunks, (((1,), (1,)), ((), ())), preferred_element_type=F32)

        @pl.when(step == 0)
        def _():
            out[...] = term

        @pl.when(step > 0)
        def _():
            out[...] += term


def values(chunks, own_rows, other_rows, steps=4):
    count, (columns, half) = chunks[0].shape[0], own_rows.shape
    depth = half // steps
    out = jax.ShapeDtypeStruct((columns, X * count), F32)
    rows = pl.BlockSpec((columns, depth), lambda i: (0, i))
    out_spec = pl.BlockSpec(out.shape, lambda i: (0, 0))
    return pl.pallas_call(
        values_kernel,
        grid=(steps,),
        in_specs=[pl.BlockSpec((count, depth), lambda i: (0, i))] * X + [rows, rows],
        out_specs=[out_spec, out_spec],
        out_shape=[out, out],
        name="values",
    )(*chunks, own_rows, other_rows)


def hidden_kernel(own_ref, other_ref, place_ref, out_ref):
    value = own_ref[...] + other_ref[...]
    width = value.shape[0] // 2
    gate_value, up_value = value[:width], value[width:]
    hidden = (gate_value / (1 + jnp.exp(-gate_value)) * up_value).astype(BF16)
    out_ref[...] = jnp.dot(hidden, place_ref[...], preferred_element_type=F32).astype(BF16)


def placed_hidden(own_value, other_value, place):
    return pl.pallas_call(
        hidden_kernel,
        out_shape=jax.ShapeDtypeStruct((own_value.shape[0] // 2, place.shape[1]), BF16),
        name="placed_hidden",
    )(own_value, other_value, place)


def block(tokens, segment_ids, gate_weight, up_weight, down_weight):
    x, gy = lax.axis_index("x"), lax.axis_index("gy")
    own_tokens, half = tokens.shape
    down = exchanged(cut_by_x(down_weight[0].T), "x")

    kinds = jnp.broadcast_to(segment_ids.astype(tokens.dtype)[:, None], (own_tokens, LANES))
    wide = jnp.concatenate([tokens, kinds], 1)
    column = lax.all_gather(wide, ("zo", "zi"), axis=0, tiled=True)
    gate, up = gate_weight[:, 0].T, up_weight[:, 0].T
    chunks = [column]
    for by in STEPS[1:]:
        chunks.append(shifted(column, "x", by))
    group = cut_by_zi(down, gy.reshape(1))
    group = exchanged(group, "zi")

    own_rows, other_rows = split_rows(gate, up, gy.reshape(1))
    other_rows = shifted(other_rows, "gy", 1)

    own_value, other_value = values(chunks, own_rows, other_rows)
    other_value = shifted(other_value, "gy", 1)
    place = placement(chunks, half, x.reshape(1), own_tokens)
    placed = placed_hidden(own_value, other_value, place)

    gathered = lax.all_gather(placed, "zo", axis=0, tiled=True)

    depth = group.shape[3]
    partial = lax.dot_general(
        gathered, group.reshape(-1, depth), (((0,), (1,)), ((), ())), preferred_element_type=F32
    )
    width = partial.shape[1] // (2 * ZI)

    def half_of(which):
        return jnp.concatenate(
            [partial[:, (2 * k + which) * width : (2 * k + which + 1) * width] for k in range(ZI)], 1
        )

    other_half = shifted(half_of(1), "gy", 1)
    summed = (half_of(0) + other_half).astype(BF16)
    slots = summed.shape[0]
    arrived = exchanged(summed.reshape(X * ZI, slots // (X * ZI), -1), ("x", "zi"))
    reduced = jnp.sum(arrived.astype(F32), axis=0).astype(BF16)
    owned = exchanged(reduced.reshape(ZO, own_tokens, -1), "zo")
    owned = owned.reshape(ZO, own_tokens, ZI, X // 2, -1).transpose(1, 3, 0, 2, 4)
    return owned.reshape(own_tokens, half)


def solution(mesh):
    torus = Mesh(
        mesh.devices.reshape(mesh.shape["rep"], X, ZO, ZI, mesh.shape["gy"]),
        ("rep", "x", "zo", "zi", "gy"),
    )
    placed = (P(REP_GX, "gy"), P(REP_GX), P(None, "gy", GX), P(None, "gy", GX), P("gy", None, GX))
    return jax.shard_map(block, mesh=torus, in_specs=placed, out_specs=P(REP_GX, "gy"), check_vma=False)
```

```python
import functools

import jax
import jax.numpy as jnp
import numpy as np
from jax import lax
from jax.experimental import pallas as pl
from jax.experimental.pallas import tpu as pltpu
from jax.sharding import Mesh
from jax.sharding import PartitionSpec as P


PREFILL = 320
X, ZO, ZI = 4, 8, 4
GX = ("x", "zo", "zi")
REP_GX = ("rep", "x", "zo", "zi")
LANES = 128
STEPS = (0, 1, 3, 2)
F32 = jnp.float32
BF16 = jnp.bfloat16


def shifted(value, axis, by):
    count = lax.axis_size(axis)
    return lax.ppermute(value, axis, [(i, (i + by) % count) for i in range(count)])


def exchanged(blocks, axes):
    return lax.all_to_all(blocks, axes, split_axis=0, concat_axis=0, tiled=True)


HBM = pl.BlockSpec(memory_space=pl.ANY)


def pass_on(ins, outs):
    for copy in ins:
        copy.start()
    for arrive, leave in zip(ins, outs, strict=True):
        arrive.wait()
        leave.start()
    for copy in outs:
        copy.wait()


def cut_by_x_kernel(rows_ref, out_ref, held, in_sems, out_sems):
    rows = out_ref.shape[2]
    ins = [
        pltpu.make_async_copy(rows_ref.at[:, pl.ds(k * rows, rows)], held.at[k], in_sems.at[k])
        for k in range(X)
    ]
    outs = [pltpu.make_async_copy(held.at[k], out_ref.at[k], out_sems.at[k]) for k in range(X)]
    pass_on(ins, outs)


def cut_by_x(down):
    features, rows = down.shape
    shape = (X, features, rows // X)
    return pl.pallas_call(
        cut_by_x_kernel,
        in_specs=[HBM],
        out_specs=HBM,
        out_shape=jax.ShapeDtypeStruct(shape, down.dtype),
        scratch_shapes=[
            pltpu.VMEM(shape, down.dtype),
            pltpu.SemaphoreType.DMA((X,)),
            pltpu.SemaphoreType.DMA((X,)),
        ],
        name="cut_by_x",
    )(down)


def split_kernel(gy_ref, gate_ref, up_ref, own_ref, other_ref, held, in_sems, out_sems):
    half = own_ref.shape[2]
    gy = gy_ref[0]
    ins, outs = [], []
    for k, ref in enumerate((gate_ref, up_ref)):
        for j, (out, which) in enumerate(((other_ref, 1 - gy), (own_ref, gy))):
            slot = 2 * k + j
            columns = pl.ds(pl.multiple_of(which * half, LANES), half)
            ins.append(pltpu.make_async_copy(ref.at[:, columns], held.at[slot], in_sems.at[slot]))
            outs.append(pltpu.make_async_copy(held.at[slot], out.at[k], out_sems.at[slot]))
    pass_on(ins, outs)


def split_rows(gate, up, gy):
    columns, both = gate.shape
    out = jax.ShapeDtypeStruct((2, columns, both // 2), gate.dtype)
    own, other = pl.pallas_call(
        split_kernel,
        in_specs=[pl.BlockSpec(memory_space=pltpu.SMEM), HBM, HBM],
        out_specs=[HBM, HBM],
        out_shape=[out, out],
        scratch_shapes=[
            pltpu.VMEM((4, columns, both // 2), gate.dtype),
            pltpu.SemaphoreType.DMA((4,)),
            pltpu.SemaphoreType.DMA((4,)),
        ],
        name="split_rows",
    )(gy, gate, up)
    return own.reshape(2 * columns, -1), other.reshape(2 * columns, -1)


def cut_kernel(depth, gy_ref, rows_ref, out_ref):
    for zi in range(ZI):
        pieces = [rows_ref[0, :, (zo * ZI + zi) * depth : (zo * ZI + zi + 1) * depth] for zo in range(ZO)]
        out_ref[zi, 0] = jnp.concatenate(pieces, axis=1)


def cut_by_zi(blocks, gy):
    count, features, rows = blocks.shape
    depth = rows // (ZO * ZI)
    return pl.pallas_call(
        functools.partial(cut_kernel, depth),
        grid_spec=pltpu.PrefetchScalarGridSpec(
            num_scalar_prefetch=1,
            grid=(count,),
            in_specs=[
                pl.BlockSpec((1, features, rows), lambda i, gy: (lax.rem(i + gy[0] * (X // 2), X), 0, 0))
            ],
            out_specs=pl.BlockSpec((ZI, 1, features, ZO * depth), lambda i, gy: (0, i, 0, 0)),
        ),
        out_shape=jax.ShapeDtypeStruct((ZI, count, features, ZO * depth), blocks.dtype),
        name="cut_by_zi",
    )(gy, blocks)


def place_kernel(x_ref, *refs):
    *kinds_refs, within_ref, within_row_ref, slot_ref, place_ref = refs
    chunk, count = kinds_refs[0].shape[0], slot_ref.shape[1]
    starts = [(lax.rem(x_ref[0] + X - by, X) * chunk).astype(F32) for by in STEPS]
    lane = lax.broadcasted_iota(jnp.int32, (1, count), 1)
    order_row = within_row_ref[...] + starts[0]
    for k in range(1, X):
        order_row = jnp.where(lane < k * chunk, order_row, within_row_ref[...] + starts[k])
    kinds = jnp.concatenate([ref[...] for ref in kinds_refs], 0)
    order = jnp.concatenate([within_ref[...] + start for start in starts], 0)
    earlier = (order_row < order[:, :1]).astype(BF16)
    decode_before = jnp.dot(earlier, kinds, preferred_element_type=F32)
    target = jnp.where(kinds.astype(F32) > 0.5, PREFILL + decode_before, order - decode_before)
    place_ref[...] = (target[:, :1] == slot_ref[...]).astype(BF16)


def placement(chunks, half, x, own_tokens):
    chunk = chunks[0].shape[0]
    count = X * chunk
    slot = np.arange(count, dtype=np.float32).reshape(X, ZO, ZI, own_tokens).transpose(0, 2, 1, 3)
    within = slot[0].reshape(chunk)
    kinds = pl.BlockSpec((chunk, LANES), lambda i: (0, half // LANES))
    row = pl.BlockSpec((1, count), lambda i: (0, 0))
    return pl.pallas_call(
        place_kernel,
        grid=(1,),
        in_specs=[pl.BlockSpec(memory_space=pltpu.SMEM)]
        + [kinds] * X
        + [pl.BlockSpec((chunk, LANES), lambda i: (0, 0)), row, row],
        out_specs=pl.BlockSpec((count, count), lambda i: (0, 0)),
        out_shape=jax.ShapeDtypeStruct((count, count), BF16),
        name="placement",
    )(
        x,
        *chunks,
        np.broadcast_to(within[:, None], (chunk, LANES)).copy(),
        np.tile(within, X).reshape(1, count),
        slot.reshape(1, count),
    )


def values_kernel(*refs):
    *chunk_refs, own_rows_ref, other_rows_ref, own_ref, other_ref = refs
    step = pl.program_id(0)
    chunks = jnp.concatenate([ref[...] for ref in chunk_refs], 0)
    for rows, out in ((other_rows_ref, other_ref), (own_rows_ref, own_ref)):
        term = lax.dot_general(rows[...], chunks, (((1,), (1,)), ((), ())), preferred_element_type=F32)

        @pl.when(step == 0)
        def _():
            out[...] = term

        @pl.when(step > 0)
        def _():
            out[...] += term


def values(chunks, own_rows, other_rows, steps=4):
    count, (columns, half) = chunks[0].shape[0], own_rows.shape
    depth = half // steps
    out = jax.ShapeDtypeStruct((columns, X * count), F32)
    rows = pl.BlockSpec((columns, depth), lambda i: (0, i))
    out_spec = pl.BlockSpec(out.shape, lambda i: (0, 0))
    return pl.pallas_call(
        values_kernel,
        grid=(steps,),
        in_specs=[pl.BlockSpec((count, depth), lambda i: (0, i))] * X + [rows, rows],
        out_specs=[out_spec, out_spec],
        out_shape=[out, out],
        name="values",
    )(*chunks, own_rows, other_rows)


def hidden_kernel(own_ref, other_ref, place_ref, out_ref):
    value = own_ref[...] + other_ref[...]
    width = value.shape[0] // 2
    gate_value, up_value = value[:width], value[width:]
    hidden = (gate_value / (1 + jnp.exp(-gate_value)) * up_value).astype(BF16)
    out_ref[...] = jnp.dot(hidden, place_ref[...], preferred_element_type=F32).astype(BF16)


def placed_hidden(own_value, other_value, place):
    return pl.pallas_call(
        hidden_kernel,
        out_shape=jax.ShapeDtypeStruct((own_value.shape[0] // 2, place.shape[1]), BF16),
        name="placed_hidden",
    )(own_value, other_value, place)


def block(tokens, segment_ids, gate_weight, up_weight, down_weight):
    x, gy = lax.axis_index("x"), lax.axis_index("gy")
    own_tokens, half = tokens.shape
    kinds = jnp.broadcast_to(segment_ids.astype(tokens.dtype)[:, None], (own_tokens, LANES))
    wide = jnp.concatenate([tokens, kinds], 1)
    copies = jnp.broadcast_to(wide, (ZO, *wide.shape))
    strided = exchanged(copies, "zo").reshape(ZO * own_tokens, -1)

    down = cut_by_x(down_weight[0].T)
    down = exchanged(down, "x")
    own_rows, other_rows = split_rows(gate_weight[:, 0].T, up_weight[:, 0].T, gy.reshape(1))
    other_rows = shifted(other_rows, "gy", 1)

    column = lax.all_gather(strided, "zi", axis=0, tiled=True)
    chunks = [column]
    for by in STEPS[1:]:
        chunks.append(shifted(column, "x", by))
    group = cut_by_zi(down, gy.reshape(1))
    group = exchanged(group, "zi")

    own_value, other_value = values(chunks, own_rows, other_rows)
    other_value = shifted(other_value, "gy", 1)
    place = placement(chunks, half, x.reshape(1), own_tokens)
    placed = placed_hidden(own_value, other_value, place)

    gathered = lax.all_gather(placed, "zo", axis=0, tiled=True)

    depth = group.shape[3]
    partial = lax.dot_general(
        gathered, group.reshape(-1, depth), (((0,), (1,)), ((), ())), preferred_element_type=F32
    )
    width = partial.shape[1] // (2 * ZI)

    def half_of(which):
        return jnp.concatenate(
            [partial[:, (2 * k + which) * width : (2 * k + which + 1) * width] for k in range(ZI)], 1
        )

    other_half = shifted(half_of(1), "gy", 1)
    summed = (half_of(0) + other_half).astype(BF16)
    slots = summed.shape[0]
    arrived = exchanged(summed.reshape(X * ZI, slots // (X * ZI), -1), ("x", "zi"))
    reduced = jnp.sum(arrived.astype(F32), axis=0).astype(BF16)
    owned = exchanged(reduced.reshape(ZO, own_tokens, -1), "zo")
    owned = owned.reshape(ZO, own_tokens, ZI, X // 2, -1).transpose(1, 3, 0, 2, 4)
    return owned.reshape(own_tokens, half)


def solution(mesh):
    torus = Mesh(
        mesh.devices.reshape(mesh.shape["rep"], X, ZO, ZI, mesh.shape["gy"]),
        ("rep", "x", "zo", "zi", "gy"),
    )
    placed = (P(REP_GX, "gy"), P(REP_GX), P(None, "gy", GX), P(None, "gy", GX), P("gy", None, GX))
    return jax.shard_map(block, mesh=torus, in_specs=placed, out_specs=P(REP_GX, "gy"), check_vma=False)
```

```python
import functools

import jax
import jax.numpy as jnp
import numpy as np
from jax import lax
from jax.experimental import pallas as pl
from jax.experimental.pallas import tpu as pltpu
from jax.sharding import Mesh
from jax.sharding import PartitionSpec as P


PREFILL = 320
X, ZO, ZI = 4, 8, 4
GX = ("x", "zo", "zi")
REP_GX = ("rep", "x", "zo", "zi")
LANES = 128
STEPS = (0, 1, 3, 2)
F32 = jnp.float32
BF16 = jnp.bfloat16


def shifted(value, axis, by):
    count = lax.axis_size(axis)
    return lax.ppermute(value, axis, [(i, (i + by) % count) for i in range(count)])


def exchanged(blocks, axes):
    return lax.all_to_all(blocks, axes, split_axis=0, concat_axis=0, tiled=True)


HBM = pl.BlockSpec(memory_space=pl.ANY)


def pass_on(ins, outs):
    for copy in ins:
        copy.start()
    for arrive, leave in zip(ins, outs, strict=True):
        arrive.wait()
        leave.start()
    for copy in outs:
        copy.wait()


def cut_by_x_kernel(x_ref, rows_ref, *refs):
    *outs, held, in_sems, out_sems = refs
    rows = held.shape[2]
    at = [pl.multiple_of(lax.rem(x_ref[0] + by, X) * rows, LANES) for by in STEPS]
    pass_on(
        [
            pltpu.make_async_copy(rows_ref.at[:, pl.ds(at[k], rows)], held.at[k], in_sems.at[k])
            for k in range(X)
        ],
        [pltpu.make_async_copy(held.at[k], outs[k], out_sems.at[k]) for k in range(X)],
    )


def cut_by_x(down, x):
    features, rows = down.shape
    out = jax.ShapeDtypeStruct((features, rows // X), down.dtype)
    return list(
        pl.pallas_call(
        cut_by_x_kernel,
        in_specs=[pl.BlockSpec(memory_space=pltpu.SMEM), HBM],
        out_specs=[HBM] * X,
        out_shape=[out] * X,
        scratch_shapes=[
            pltpu.VMEM((X, *out.shape), down.dtype),
            pltpu.SemaphoreType.DMA((X,)),
            pltpu.SemaphoreType.DMA((X,)),
        ],
        name="cut_by_x",
    )(x, down))


def split_kernel(gy_ref, gate_ref, up_ref, own_ref, other_ref, held, in_sems, out_sems):
    half = own_ref.shape[2]
    gy = gy_ref[0]
    ins, outs = [], []
    for k, ref in enumerate((gate_ref, up_ref)):
        for j, (out, which) in enumerate(((other_ref, 1 - gy), (own_ref, gy))):
            slot = 2 * k + j
            columns = pl.ds(pl.multiple_of(which * half, LANES), half)
            ins.append(pltpu.make_async_copy(ref.at[:, columns], held.at[slot], in_sems.at[slot]))
            outs.append(pltpu.make_async_copy(held.at[slot], out.at[k], out_sems.at[slot]))
    pass_on(ins, outs)


def split_rows(gate, up, gy):
    columns, both = gate.shape
    out = jax.ShapeDtypeStruct((2, columns, both // 2), gate.dtype)
    own, other = pl.pallas_call(
        split_kernel,
        in_specs=[pl.BlockSpec(memory_space=pltpu.SMEM), HBM, HBM],
        out_specs=[HBM, HBM],
        out_shape=[out, out],
        scratch_shapes=[
            pltpu.VMEM((4, columns, both // 2), gate.dtype),
            pltpu.SemaphoreType.DMA((4,)),
            pltpu.SemaphoreType.DMA((4,)),
        ],
        name="split_rows",
    )(gy, gate, up)
    return own.reshape(2 * columns, -1), other.reshape(2 * columns, -1)


def cut_by_zi_kernel(depth, x_ref, gy_ref, *refs):
    *rows_refs, out_ref = refs
    for by, rows_ref in zip(STEPS, rows_refs, strict=True):
        position = lax.rem(x_ref[0] + 2 * X - by - gy_ref[0] * (X // 2), X)
        for zi in range(ZI):
            pieces = [rows_ref[:, (zo * ZI + zi) * depth : (zo * ZI + zi + 1) * depth] for zo in range(ZO)]
            out_ref[zi, position] = jnp.concatenate(pieces, axis=1)


def cut_by_zi(blocks, x, gy):
    features, rows = blocks[0].shape
    depth = rows // (ZO * ZI)
    scalar = pl.BlockSpec(memory_space=pltpu.SMEM)
    whole = pl.BlockSpec(memory_space=pltpu.VMEM)
    return pl.pallas_call(
        functools.partial(cut_by_zi_kernel, depth),
        in_specs=[scalar, scalar] + [whole] * X,
        out_specs=whole,
        out_shape=jax.ShapeDtypeStruct((ZI, X, features, ZO * depth), blocks[0].dtype),
        name="cut_by_zi",
    )(x, gy, *blocks)


def place_kernel(x_ref, *refs):
    *kinds_refs, within_ref, within_row_ref, slot_ref, place_ref = refs
    chunk, count = kinds_refs[0].shape[0], slot_ref.shape[1]
    starts = [(lax.rem(x_ref[0] + X - by, X) * chunk).astype(F32) for by in STEPS]
    lane = lax.broadcasted_iota(jnp.int32, (1, count), 1)
    order_row = within_row_ref[...] + starts[0]
    for k in range(1, X):
        order_row = jnp.where(lane < k * chunk, order_row, within_row_ref[...] + starts[k])
    kinds = jnp.concatenate([ref[...] for ref in kinds_refs], 0)
    order = jnp.concatenate([within_ref[...] + start for start in starts], 0)
    earlier = (order_row < order[:, :1]).astype(BF16)
    decode_before = jnp.dot(earlier, kinds, preferred_element_type=F32)
    target = jnp.where(kinds.astype(F32) > 0.5, PREFILL + decode_before, order - decode_before)
    place_ref[...] = (target[:, :1] == slot_ref[...]).astype(BF16)


def placement(chunks, half, x, own_tokens):
    chunk = chunks[0].shape[0]
    count = X * chunk
    slot = np.arange(count, dtype=np.float32).reshape(X, ZO, ZI, own_tokens).transpose(0, 2, 1, 3)
    within = slot[0].reshape(chunk)
    kinds = pl.BlockSpec((chunk, LANES), lambda i: (0, half // LANES))
    row = pl.BlockSpec((1, count), lambda i: (0, 0))
    return pl.pallas_call(
        place_kernel,
        grid=(1,),
        in_specs=[pl.BlockSpec(memory_space=pltpu.SMEM)]
        + [kinds] * X
        + [pl.BlockSpec((chunk, LANES), lambda i: (0, 0)), row, row],
        out_specs=pl.BlockSpec((count, count), lambda i: (0, 0)),
        out_shape=jax.ShapeDtypeStruct((count, count), BF16),
        name="placement",
    )(
        x,
        *chunks,
        np.broadcast_to(within[:, None], (chunk, LANES)).copy(),
        np.tile(within, X).reshape(1, count),
        slot.reshape(1, count),
    )


def values_kernel(*refs):
    *chunk_refs, own_rows_ref, other_rows_ref, own_ref, other_ref = refs
    step = pl.program_id(0)
    chunks = jnp.concatenate([ref[...] for ref in chunk_refs], 0)
    for rows, out in ((other_rows_ref, other_ref), (own_rows_ref, own_ref)):
        term = lax.dot_general(rows[...], chunks, (((1,), (1,)), ((), ())), preferred_element_type=F32)

        @pl.when(step == 0)
        def _():
            out[...] = term

        @pl.when(step > 0)
        def _():
            out[...] += term


def values(chunks, own_rows, other_rows, steps=4):
    count, (columns, half) = chunks[0].shape[0], own_rows.shape
    depth = half // steps
    out = jax.ShapeDtypeStruct((columns, X * count), F32)
    rows = pl.BlockSpec((columns, depth), lambda i: (0, i))
    out_spec = pl.BlockSpec(out.shape, lambda i: (0, 0))
    return pl.pallas_call(
        values_kernel,
        grid=(steps,),
        in_specs=[pl.BlockSpec((count, depth), lambda i: (0, i))] * X + [rows, rows],
        out_specs=[out_spec, out_spec],
        out_shape=[out, out],
        name="values",
    )(*chunks, own_rows, other_rows)


def hidden_kernel(own_ref, other_ref, place_ref, out_ref):
    value = own_ref[...] + other_ref[...]
    width = value.shape[0] // 2
    gate_value, up_value = value[:width], value[width:]
    hidden = (gate_value / (1 + jnp.exp(-gate_value)) * up_value).astype(BF16)
    out_ref[...] = jnp.dot(hidden, place_ref[...], preferred_element_type=F32).astype(BF16)


def placed_hidden(own_value, other_value, place):
    return pl.pallas_call(
        hidden_kernel,
        out_shape=jax.ShapeDtypeStruct((own_value.shape[0] // 2, place.shape[1]), BF16),
        name="placed_hidden",
    )(own_value, other_value, place)


def block(tokens, segment_ids, gate_weight, up_weight, down_weight):
    x, gy = lax.axis_index("x"), lax.axis_index("gy")
    own_tokens, half = tokens.shape
    kinds = jnp.broadcast_to(segment_ids.astype(tokens.dtype)[:, None], (own_tokens, LANES))
    wide = jnp.concatenate([tokens, kinds], 1)
    copies = jnp.broadcast_to(wide, (ZO, *wide.shape))
    strided = exchanged(copies, "zo").reshape(ZO * own_tokens, -1)

    x_at, gy_at = x.reshape(1), gy.reshape(1)
    blocks = cut_by_x(down_weight[0].T, x_at)
    for k in range(1, X):
        blocks[k] = shifted(blocks[k], "x", STEPS[k])
    own_rows, other_rows = split_rows(gate_weight[:, 0].T, up_weight[:, 0].T, gy_at)
    other_rows = shifted(other_rows, "gy", 1)
    other_rows, *blocks = lax.optimization_barrier((other_rows, *blocks))
    group = cut_by_zi(blocks, x_at, gy_at)

    column = lax.all_gather(strided, "zi", axis=0, tiled=True)
    chunks = [column]
    for by in STEPS[1:]:
        chunks.append(shifted(column, "x", by))
    group = exchanged(group, "zi")

    own_value, other_value = values(chunks, own_rows, other_rows)
    other_value = shifted(other_value, "gy", 1)
    place = placement(chunks, half, x_at, own_tokens)
    placed = placed_hidden(own_value, other_value, place)

    gathered = lax.all_gather(placed, "zo", axis=0, tiled=True)

    depth = group.shape[3]
    partial = lax.dot_general(
        gathered, group.reshape(-1, depth), (((0,), (1,)), ((), ())), preferred_element_type=F32
    )
    width = partial.shape[1] // (2 * ZI)

    def half_of(which):
        return jnp.concatenate(
            [partial[:, (2 * k + which) * width : (2 * k + which + 1) * width] for k in range(ZI)], 1
        )

    other_half = shifted(half_of(1), "gy", 1)
    summed = (half_of(0) + other_half).astype(BF16)
    slots = summed.shape[0]
    arrived = exchanged(summed.reshape(X * ZI, slots // (X * ZI), -1), ("x", "zi"))
    reduced = jnp.sum(arrived.astype(F32), axis=0).astype(BF16)
    owned = exchanged(reduced.reshape(ZO, own_tokens, -1), "zo")
    owned = owned.reshape(ZO, own_tokens, ZI, X // 2, -1).transpose(1, 3, 0, 2, 4)
    return owned.reshape(own_tokens, half)


def solution(mesh):
    torus = Mesh(
        mesh.devices.reshape(mesh.shape["rep"], X, ZO, ZI, mesh.shape["gy"]),
        ("rep", "x", "zo", "zi", "gy"),
    )
    placed = (P(REP_GX, "gy"), P(REP_GX), P(None, "gy", GX), P(None, "gy", GX), P("gy", None, GX))
    return jax.shard_map(
        block, mesh=torus, in_specs=placed, out_specs=P(REP_GX, "gy"), check_vma=False
    )
```

```python
import functools

import jax
import jax.numpy as jnp
import numpy as np
from jax import lax
from jax.experimental import pallas as pl
from jax.experimental.pallas import tpu as pltpu
from jax.sharding import Mesh
from jax.sharding import PartitionSpec as P


PREFILL = 320
X, ZO, ZI = 4, 8, 4
GX = ("x", "zo", "zi")
REP_GX = ("rep", "x", "zo", "zi")
LANES = 128
STEPS = (0, 1, 3, 2)
F32 = jnp.float32
BF16 = jnp.bfloat16


def shifted(value, axis, by):
    count = lax.axis_size(axis)
    return lax.ppermute(value, axis, [(i, (i + by) % count) for i in range(count)])


def exchanged(blocks, axes):
    return lax.all_to_all(blocks, axes, split_axis=0, concat_axis=0, tiled=True)


HBM = pl.BlockSpec(memory_space=pl.ANY)


def pass_on(ins, outs):
    for copy in ins:
        copy.start()
    for arrive, leave in zip(ins, outs, strict=True):
        arrive.wait()
        leave.start()
    for copy in outs:
        copy.wait()


def copies_kernel(kinds_ref, tokens_ref, out_ref):
    count, half = tokens_ref.shape
    row = lax.broadcasted_iota(jnp.int32, (count, LANES), 0)
    kinds = jnp.zeros((count, LANES), F32)
    for k in range(count):
        kinds = jnp.where(row == k, kinds_ref[k].astype(F32), kinds)
    for k in range(ZO):
        out_ref[k, :, :half] = tokens_ref[...]
        out_ref[k, :, half:] = kinds.astype(BF16)


def token_copies(tokens, segment_ids):
    count, half = tokens.shape
    return pl.pallas_call(
        copies_kernel,
        in_specs=[pl.BlockSpec(memory_space=pltpu.SMEM), pl.BlockSpec(memory_space=pltpu.VMEM)],
        out_specs=pl.BlockSpec(memory_space=pltpu.VMEM),
        out_shape=jax.ShapeDtypeStruct((ZO, count, half + LANES), tokens.dtype),
        name="token_copies",
    )(segment_ids, tokens)


def cut_by_x_kernel(x_ref, rows_ref, *refs):
    *outs, held, in_sems, out_sems = refs
    rows = held.shape[2]
    at = [pl.multiple_of(lax.rem(x_ref[0] + by, X) * rows, LANES) for by in STEPS]
    pass_on(
        [
            pltpu.make_async_copy(rows_ref.at[:, pl.ds(at[k], rows)], held.at[k], in_sems.at[k])
            for k in range(X)
        ],
        [pltpu.make_async_copy(held.at[k], outs[k], out_sems.at[k]) for k in range(X)],
    )


def cut_by_x(down, x):
    features, rows = down.shape
    out = jax.ShapeDtypeStruct((features, rows // X), down.dtype)
    blocks = pl.pallas_call(
        cut_by_x_kernel,
        in_specs=[pl.BlockSpec(memory_space=pltpu.SMEM), HBM],
        out_specs=[HBM] * X,
        out_shape=[out] * X,
        scratch_shapes=[
            pltpu.VMEM((X, *out.shape), down.dtype),
            pltpu.SemaphoreType.DMA((X,)),
            pltpu.SemaphoreType.DMA((X,)),
        ],
        name="cut_by_x",
    )(x, down)
    return list(blocks)


def split_kernel(gy_ref, gate_ref, up_ref, own_ref, other_ref, held, in_sems, out_sems):
    half = own_ref.shape[2]
    gy = gy_ref[0]
    ins, outs = [], []
    for k, ref in enumerate((gate_ref, up_ref)):
        for j, (out, which) in enumerate(((other_ref, 1 - gy), (own_ref, gy))):
            slot = 2 * k + j
            columns = pl.ds(pl.multiple_of(which * half, LANES), half)
            ins.append(pltpu.make_async_copy(ref.at[:, columns], held.at[slot], in_sems.at[slot]))
            outs.append(pltpu.make_async_copy(held.at[slot], out.at[k], out_sems.at[slot]))
    pass_on(ins, outs)


def split_rows(gate, up, gy):
    columns, both = gate.shape
    out = jax.ShapeDtypeStruct((2, columns, both // 2), gate.dtype)
    own, other = pl.pallas_call(
        split_kernel,
        in_specs=[pl.BlockSpec(memory_space=pltpu.SMEM), HBM, HBM],
        out_specs=[HBM, HBM],
        out_shape=[out, out],
        scratch_shapes=[
            pltpu.VMEM((4, columns, both // 2), gate.dtype),
            pltpu.SemaphoreType.DMA((4,)),
            pltpu.SemaphoreType.DMA((4,)),
        ],
        name="split_rows",
    )(gy, gate, up)
    return own.reshape(2 * columns, -1), other.reshape(2 * columns, -1)


def cut_by_zi_kernel(depth, x_ref, gy_ref, *refs):
    *rows_refs, out_ref = refs
    for by, rows_ref in zip(STEPS, rows_refs, strict=True):
        position = lax.rem(x_ref[0] + 2 * X - by - gy_ref[0] * (X // 2), X)
        for zi in range(ZI):
            pieces = [rows_ref[:, (zo * ZI + zi) * depth : (zo * ZI + zi + 1) * depth] for zo in range(ZO)]
            out_ref[zi, position] = jnp.concatenate(pieces, axis=1)


def cut_by_zi(blocks, x, gy):
    features, rows = blocks[0].shape
    depth = rows // (ZO * ZI)
    scalar = pl.BlockSpec(memory_space=pltpu.SMEM)
    whole = pl.BlockSpec(memory_space=pltpu.VMEM)
    return pl.pallas_call(
        functools.partial(cut_by_zi_kernel, depth),
        in_specs=[scalar, scalar] + [whole] * X,
        out_specs=whole,
        out_shape=jax.ShapeDtypeStruct((ZI, X, features, ZO * depth), blocks[0].dtype),
        name="cut_by_zi",
    )(x, gy, *blocks)


def place_kernel(x_ref, *refs):
    *kinds_refs, within_ref, within_row_ref, slot_ref, place_ref = refs
    chunk, count = kinds_refs[0].shape[0], slot_ref.shape[1]
    starts = [(lax.rem(x_ref[0] + X - by, X) * chunk).astype(F32) for by in STEPS]
    lane = lax.broadcasted_iota(jnp.int32, (1, count), 1)
    order_row = within_row_ref[...] + starts[0]
    for k in range(1, X):
        order_row = jnp.where(lane < k * chunk, order_row, within_row_ref[...] + starts[k])
    kinds = jnp.concatenate([ref[...] for ref in kinds_refs], 0)
    order = jnp.concatenate([within_ref[...] + start for start in starts], 0)
    earlier = (order_row < order[:, :1]).astype(BF16)
    decode_before = jnp.dot(earlier, kinds, preferred_element_type=F32)
    target = jnp.where(kinds.astype(F32) > 0.5, PREFILL + decode_before, order - decode_before)
    place_ref[...] = (target[:, :1] == slot_ref[...]).astype(BF16)


def placement(chunks, half, x, own_tokens):
    chunk = chunks[0].shape[0]
    count = X * chunk
    slot = np.arange(count, dtype=np.float32).reshape(X, ZO, ZI, own_tokens).transpose(0, 2, 1, 3)
    within = slot[0].reshape(chunk)
    kinds = pl.BlockSpec((chunk, LANES), lambda i: (0, half // LANES))
    row = pl.BlockSpec((1, count), lambda i: (0, 0))
    return pl.pallas_call(
        place_kernel,
        grid=(1,),
        in_specs=[pl.BlockSpec(memory_space=pltpu.SMEM)]
        + [kinds] * X
        + [pl.BlockSpec((chunk, LANES), lambda i: (0, 0)), row, row],
        out_specs=pl.BlockSpec((count, count), lambda i: (0, 0)),
        out_shape=jax.ShapeDtypeStruct((count, count), BF16),
        name="placement",
    )(
        x,
        *chunks,
        np.broadcast_to(within[:, None], (chunk, LANES)).copy(),
        np.tile(within, X).reshape(1, count),
        slot.reshape(1, count),
    )


def values_kernel(*refs):
    *chunk_refs, own_rows_ref, other_rows_ref, own_ref, other_ref = refs
    step = pl.program_id(0)
    columns = own_rows_ref.shape[0]
    chunks = jnp.concatenate([ref[...] for ref in chunk_refs], 0)
    rows = jnp.concatenate([own_rows_ref[...], other_rows_ref[...]], 0)
    term = lax.dot_general(rows, chunks, (((1,), (1,)), ((), ())), preferred_element_type=F32)

    @pl.when(step == 0)
    def _():
        own_ref[...] = term[:columns]
        other_ref[...] = term[columns:]

    @pl.when(step > 0)
    def _():
        own_ref[...] += term[:columns]
        other_ref[...] += term[columns:]


def values(chunks, own_rows, other_rows, steps=2):
    columns, half = own_rows.shape
    count = sum(chunk.shape[0] for chunk in chunks)
    depth = half // steps
    out = jax.ShapeDtypeStruct((columns, count), F32)
    rows = pl.BlockSpec((columns, depth), lambda i: (0, i))
    out_spec = pl.BlockSpec(out.shape, lambda i: (0, 0))
    return pl.pallas_call(
        values_kernel,
        grid=(steps,),
        in_specs=[pl.BlockSpec((chunk.shape[0], depth), lambda i: (0, i)) for chunk in chunks] + [rows, rows],
        out_specs=[out_spec, out_spec],
        out_shape=[out, out],
        name="values",
    )(*chunks, own_rows, other_rows)


def hidden_kernel(own_ref, other_ref, place_ref, out_ref):
    value = own_ref[...] + other_ref[...]
    width = value.shape[0] // 2
    gate_value, up_value = value[:width], value[width:]
    hidden = (gate_value / (1 + jnp.exp(-gate_value)) * up_value).astype(BF16)
    out_ref[...] = jnp.dot(hidden, place_ref[...], preferred_element_type=F32).astype(BF16)


def placed_hidden(own_value, other_value, place):
    return pl.pallas_call(
        hidden_kernel,
        out_shape=jax.ShapeDtypeStruct((own_value.shape[0] // 2, place.shape[1]), BF16),
        name="placed_hidden",
    )(own_value, other_value, place)


def block(tokens, segment_ids, gate_weight, up_weight, down_weight):
    x, gy = lax.axis_index("x"), lax.axis_index("gy")
    own_tokens, half = tokens.shape
    copies = token_copies(tokens, segment_ids)
    strided = exchanged(copies, "zo").reshape(ZO * own_tokens, -1)

    x_at, gy_at = x.reshape(1), gy.reshape(1)
    blocks = cut_by_x(down_weight[0].T, x_at)
    for k in range(1, X):
        blocks[k] = shifted(blocks[k], "x", STEPS[k])
    own_rows, other_rows = split_rows(gate_weight[:, 0].T, up_weight[:, 0].T, gy_at)
    other_rows = shifted(other_rows, "gy", 1)
    other_rows, *blocks = lax.optimization_barrier((other_rows, *blocks))
    group = cut_by_zi(blocks, x_at, gy_at)

    column = lax.all_gather(strided, "zi", axis=0, tiled=True)
    chunks = [column]
    for by in STEPS[1:]:
        chunks.append(shifted(column, "x", by))
    group = exchanged(group, "zi")

    own_value, other_value = values(chunks, own_rows, other_rows)
    other_value = shifted(other_value, "gy", 1)
    place = placement(chunks, half, x_at, own_tokens)
    placed = placed_hidden(own_value, other_value, place)

    gathered = lax.all_gather(placed, "zo", axis=0, tiled=True)

    depth = group.shape[3]
    partial = lax.dot_general(
        gathered, group.reshape(-1, depth), (((0,), (1,)), ((), ())), preferred_element_type=F32
    )
    width = partial.shape[1] // (2 * ZI)

    def half_of(which):
        return jnp.concatenate(
            [partial[:, (2 * k + which) * width : (2 * k + which + 1) * width] for k in range(ZI)], 1
        )

    other_half = shifted(half_of(1), "gy", 1)
    summed = (half_of(0) + other_half).astype(BF16)
    slots = summed.shape[0]
    arrived = exchanged(summed.reshape(X * ZI, slots // (X * ZI), -1), ("x", "zi"))
    reduced = jnp.sum(arrived.astype(F32), axis=0).astype(BF16)
    owned = exchanged(reduced.reshape(ZO, own_tokens, -1), "zo")
    owned = owned.reshape(ZO, own_tokens, ZI, X // 2, -1).transpose(1, 3, 0, 2, 4)
    return owned.reshape(own_tokens, half)


def solution(mesh):
    torus = Mesh(
        mesh.devices.reshape(mesh.shape["rep"], X, ZO, ZI, mesh.shape["gy"]),
        ("rep", "x", "zo", "zi", "gy"),
    )
    placed = (P(REP_GX, "gy"), P(REP_GX), P(None, "gy", GX), P(None, "gy", GX), P("gy", None, GX))
    return jax.shard_map(
        block, mesh=torus, in_specs=placed, out_specs=P(REP_GX, "gy"), check_vma=False
    )
```

```python
import functools

import jax
import jax.numpy as jnp
import numpy as np
from jax import lax
from jax.experimental import pallas as pl
from jax.experimental.pallas import tpu as pltpu
from jax.sharding import Mesh
from jax.sharding import PartitionSpec as P


PREFILL = 320
X, ZO, ZI = 4, 8, 4
GX = ("x", "zo", "zi")
REP_GX = ("rep", "x", "zo", "zi")
SUBLANES, LANES = 8, 128
STEPS = (0, 1, 3, 2)
F32 = jnp.float32
BF16 = jnp.bfloat16


def shifted(value, axis, by):
    count = lax.axis_size(axis)
    return lax.ppermute(value, axis, [(i, (i + by) % count) for i in range(count)])


def exchanged(blocks, axes):
    return lax.all_to_all(blocks, axes, split_axis=0, concat_axis=0, tiled=True)


HBM = pl.BlockSpec(memory_space=pl.ANY)


def pass_on(ins, outs):
    for copy in ins:
        copy.start()
    for arrive, leave in zip(ins, outs, strict=True):
        arrive.wait()
        leave.start()
    for copy in outs:
        copy.wait()


def pack_kernel(kinds_ref, tokens_ref, out_ref):
    count, half = tokens_ref.shape
    piece = half // SUBLANES
    tokens = tokens_ref[...].astype(F32)
    rows = [
        jnp.concatenate([tokens[k : k + 1, e * piece : (e + 1) * piece] for k in range(count)], 1)
        for e in range(SUBLANES)
    ]
    packed = jnp.concatenate(rows, 0).astype(BF16)
    row = lax.broadcasted_iota(jnp.int32, (SUBLANES, LANES), 0)
    kinds = jnp.zeros((SUBLANES, LANES), F32)
    for k in range(count):
        kinds = jnp.where(row == k, kinds_ref[k].astype(F32), kinds)
    for k in range(ZO):
        out_ref[k, :, : count * piece] = packed
        out_ref[k, :, count * piece :] = kinds.astype(BF16)


def packed_tokens(tokens, segment_ids):
    count, half = tokens.shape
    return pl.pallas_call(
        pack_kernel,
        in_specs=[pl.BlockSpec(memory_space=pltpu.SMEM), pl.BlockSpec(memory_space=pltpu.VMEM)],
        out_specs=pl.BlockSpec(memory_space=pltpu.VMEM),
        out_shape=jax.ShapeDtypeStruct((ZO, SUBLANES, count * half // SUBLANES + LANES), tokens.dtype),
        name="packed_tokens",
    )(segment_ids, tokens)


def unpack_kernel(count, packed_ref, out_ref):
    piece = (packed_ref.shape[2] - LANES) // count
    rows = []
    for zo in range(ZO):
        packed = packed_ref[zo].astype(F32)
        for k in range(count):
            parts = [packed[e : e + 1, k * piece : (k + 1) * piece] for e in range(SUBLANES)]
            rows.append(jnp.concatenate(parts + [packed[k : k + 1, count * piece :]], 1))
    out_ref[...] = jnp.concatenate(rows, 0).astype(BF16)


def unpacked_tokens(packed, count):
    columns = (packed.shape[2] - LANES) // count * SUBLANES + LANES
    return pl.pallas_call(
        functools.partial(unpack_kernel, count),
        in_specs=[pl.BlockSpec(memory_space=pltpu.VMEM)],
        out_specs=pl.BlockSpec(memory_space=pltpu.VMEM),
        out_shape=jax.ShapeDtypeStruct((ZO * count, columns), packed.dtype),
        name="unpacked_tokens",
    )(packed)


def cut_by_x_kernel(x_ref, rows_ref, *refs):
    *outs, held, in_sems, out_sems = refs
    rows = held.shape[2]
    at = [pl.multiple_of(lax.rem(x_ref[0] + by, X) * rows, LANES) for by in STEPS]
    pass_on(
        [
            pltpu.make_async_copy(rows_ref.at[:, pl.ds(at[k], rows)], held.at[k], in_sems.at[k])
            for k in range(X)
        ],
        [pltpu.make_async_copy(held.at[k], outs[k], out_sems.at[k]) for k in range(X)],
    )


def cut_by_x(down, x):
    features, rows = down.shape
    out = jax.ShapeDtypeStruct((features, rows // X), down.dtype)
    blocks = pl.pallas_call(
        cut_by_x_kernel,
        in_specs=[pl.BlockSpec(memory_space=pltpu.SMEM), HBM],
        out_specs=[HBM] * X,
        out_shape=[out] * X,
        scratch_shapes=[
            pltpu.VMEM((X, *out.shape), down.dtype),
            pltpu.SemaphoreType.DMA((X,)),
            pltpu.SemaphoreType.DMA((X,)),
        ],
        name="cut_by_x",
    )(x, down)
    return list(blocks)


def split_kernel(gy_ref, gate_ref, up_ref, own_ref, other_ref, held, in_sems, out_sems):
    half = own_ref.shape[2]
    gy = gy_ref[0]
    ins, outs = [], []
    for k, ref in enumerate((gate_ref, up_ref)):
        for j, (out, which) in enumerate(((other_ref, 1 - gy), (own_ref, gy))):
            slot = 2 * k + j
            columns = pl.ds(pl.multiple_of(which * half, LANES), half)
            ins.append(pltpu.make_async_copy(ref.at[:, columns], held.at[slot], in_sems.at[slot]))
            outs.append(pltpu.make_async_copy(held.at[slot], out.at[k], out_sems.at[slot]))
    pass_on(ins, outs)


def split_rows(gate, up, gy):
    columns, both = gate.shape
    out = jax.ShapeDtypeStruct((2, columns, both // 2), gate.dtype)
    own, other = pl.pallas_call(
        split_kernel,
        in_specs=[pl.BlockSpec(memory_space=pltpu.SMEM), HBM, HBM],
        out_specs=[HBM, HBM],
        out_shape=[out, out],
        scratch_shapes=[
            pltpu.VMEM((4, columns, both // 2), gate.dtype),
            pltpu.SemaphoreType.DMA((4,)),
            pltpu.SemaphoreType.DMA((4,)),
        ],
        name="split_rows",
    )(gy, gate, up)
    return own.reshape(2 * columns, -1), other.reshape(2 * columns, -1)


def cut_by_zi_kernel(depth, x_ref, gy_ref, *refs):
    *rows_refs, out_ref = refs
    for by, rows_ref in zip(STEPS, rows_refs, strict=True):
        position = lax.rem(x_ref[0] + 2 * X - by - gy_ref[0] * (X // 2), X)
        for zi in range(ZI):
            pieces = [rows_ref[:, (zo * ZI + zi) * depth : (zo * ZI + zi + 1) * depth] for zo in range(ZO)]
            out_ref[zi, position] = jnp.concatenate(pieces, axis=1)


def cut_by_zi(blocks, x, gy):
    features, rows = blocks[0].shape
    depth = rows // (ZO * ZI)
    scalar = pl.BlockSpec(memory_space=pltpu.SMEM)
    whole = pl.BlockSpec(memory_space=pltpu.VMEM)
    return pl.pallas_call(
        functools.partial(cut_by_zi_kernel, depth),
        in_specs=[scalar, scalar] + [whole] * X,
        out_specs=whole,
        out_shape=jax.ShapeDtypeStruct((ZI, X, features, ZO * depth), blocks[0].dtype),
        name="cut_by_zi",
    )(x, gy, *blocks)


def place_kernel(x_ref, *refs):
    *kinds_refs, within_ref, within_row_ref, slot_ref, place_ref = refs
    chunk, count = kinds_refs[0].shape[0], slot_ref.shape[1]
    starts = [(lax.rem(x_ref[0] + X - by, X) * chunk).astype(F32) for by in STEPS]
    lane = lax.broadcasted_iota(jnp.int32, (1, count), 1)
    order_row = within_row_ref[...] + starts[0]
    for k in range(1, X):
        order_row = jnp.where(lane < k * chunk, order_row, within_row_ref[...] + starts[k])
    kinds = jnp.concatenate([ref[...] for ref in kinds_refs], 0)
    order = jnp.concatenate([within_ref[...] + start for start in starts], 0)
    earlier = (order_row < order[:, :1]).astype(BF16)
    decode_before = jnp.dot(earlier, kinds, preferred_element_type=F32)
    target = jnp.where(kinds.astype(F32) > 0.5, PREFILL + decode_before, order - decode_before)
    place_ref[...] = (target[:, :1] == slot_ref[...]).astype(BF16)


def placement(chunks, half, x, own_tokens):
    chunk = chunks[0].shape[0]
    count = X * chunk
    slot = np.arange(count, dtype=np.float32).reshape(X, ZO, ZI, own_tokens).transpose(0, 2, 1, 3)
    within = slot[0].reshape(chunk)
    kinds = pl.BlockSpec((chunk, LANES), lambda i: (0, half // LANES))
    row = pl.BlockSpec((1, count), lambda i: (0, 0))
    return pl.pallas_call(
        place_kernel,
        grid=(1,),
        in_specs=[pl.BlockSpec(memory_space=pltpu.SMEM)]
        + [kinds] * X
        + [pl.BlockSpec((chunk, LANES), lambda i: (0, 0)), row, row],
        out_specs=pl.BlockSpec((count, count), lambda i: (0, 0)),
        out_shape=jax.ShapeDtypeStruct((count, count), BF16),
        name="placement",
    )(
        x,
        *chunks,
        np.broadcast_to(within[:, None], (chunk, LANES)).copy(),
        np.tile(within, X).reshape(1, count),
        slot.reshape(1, count),
    )


def values_kernel(*refs):
    *chunk_refs, own_rows_ref, other_rows_ref, own_ref, other_ref = refs
    step = pl.program_id(0)
    columns = own_rows_ref.shape[0]
    chunks = jnp.concatenate([ref[...] for ref in chunk_refs], 0)
    rows = jnp.concatenate([own_rows_ref[...], other_rows_ref[...]], 0)
    term = lax.dot_general(rows, chunks, (((1,), (1,)), ((), ())), preferred_element_type=F32)

    @pl.when(step == 0)
    def _():
        own_ref[...] = term[:columns]
        other_ref[...] = term[columns:]

    @pl.when(step > 0)
    def _():
        own_ref[...] += term[:columns]
        other_ref[...] += term[columns:]


def values(chunks, own_rows, other_rows, steps=2):
    columns, half = own_rows.shape
    count = sum(chunk.shape[0] for chunk in chunks)
    depth = half // steps
    out = jax.ShapeDtypeStruct((columns, count), F32)
    rows = pl.BlockSpec((columns, depth), lambda i: (0, i))
    out_spec = pl.BlockSpec(out.shape, lambda i: (0, 0))
    return pl.pallas_call(
        values_kernel,
        grid=(steps,),
        in_specs=[pl.BlockSpec((chunk.shape[0], depth), lambda i: (0, i)) for chunk in chunks] + [rows, rows],
        out_specs=[out_spec, out_spec],
        out_shape=[out, out],
        name="values",
    )(*chunks, own_rows, other_rows)


def hidden_kernel(own_ref, other_ref, place_ref, out_ref):
    value = own_ref[...] + other_ref[...]
    width = value.shape[0] // 2
    gate_value, up_value = value[:width], value[width:]
    hidden = (gate_value / (1 + jnp.exp(-gate_value)) * up_value).astype(BF16)
    out_ref[...] = jnp.dot(hidden, place_ref[...], preferred_element_type=F32).astype(BF16)


def placed_hidden(own_value, other_value, place):
    return pl.pallas_call(
        hidden_kernel,
        out_shape=jax.ShapeDtypeStruct((own_value.shape[0] // 2, place.shape[1]), BF16),
        name="placed_hidden",
    )(own_value, other_value, place)


def block(tokens, segment_ids, gate_weight, up_weight, down_weight):
    x, gy = lax.axis_index("x"), lax.axis_index("gy")
    own_tokens, half = tokens.shape
    packed = exchanged(packed_tokens(tokens, segment_ids), "zo")
    strided = unpacked_tokens(packed, own_tokens)

    x_at, gy_at = x.reshape(1), gy.reshape(1)
    blocks = cut_by_x(down_weight[0].T, x_at)
    for k in range(1, X):
        blocks[k] = shifted(blocks[k], "x", STEPS[k])
    own_rows, other_rows = split_rows(gate_weight[:, 0].T, up_weight[:, 0].T, gy_at)
    other_rows = shifted(other_rows, "gy", 1)
    other_rows, *blocks = lax.optimization_barrier((other_rows, *blocks))
    group = cut_by_zi(blocks, x_at, gy_at)

    column = lax.all_gather(strided, "zi", axis=0, tiled=True)
    chunks = [column]
    for by in STEPS[1:]:
        chunks.append(shifted(column, "x", by))
    group = exchanged(group, "zi")

    own_value, other_value = values(chunks, own_rows, other_rows)
    other_value = shifted(other_value, "gy", 1)
    place = placement(chunks, half, x_at, own_tokens)
    placed = placed_hidden(own_value, other_value, place)

    gathered = lax.all_gather(placed, "zo", axis=0, tiled=True)

    depth = group.shape[3]
    partial = lax.dot_general(
        gathered, group.reshape(-1, depth), (((0,), (1,)), ((), ())), preferred_element_type=F32
    )
    width = partial.shape[1] // (2 * ZI)

    def half_of(which):
        return jnp.concatenate(
            [partial[:, (2 * k + which) * width : (2 * k + which + 1) * width] for k in range(ZI)], 1
        )

    other_half = shifted(half_of(1), "gy", 1)
    summed = (half_of(0) + other_half).astype(BF16)
    slots = summed.shape[0]
    arrived = exchanged(summed.reshape(X * ZI, slots // (X * ZI), -1), ("x", "zi"))
    reduced = jnp.sum(arrived.astype(F32), axis=0).astype(BF16)
    owned = exchanged(reduced.reshape(ZO, own_tokens, -1), "zo")
    owned = owned.reshape(ZO, own_tokens, ZI, X // 2, -1).transpose(1, 3, 0, 2, 4)
    return owned.reshape(own_tokens, half)


def solution(mesh):
    torus = Mesh(
        mesh.devices.reshape(mesh.shape["rep"], X, ZO, ZI, mesh.shape["gy"]),
        ("rep", "x", "zo", "zi", "gy"),
    )
    placed = (P(REP_GX, "gy"), P(REP_GX), P(None, "gy", GX), P(None, "gy", GX), P("gy", None, GX))
    return jax.shard_map(block, mesh=torus, in_specs=placed, out_specs=P(REP_GX, "gy"), check_vma=False)
```

```python
import functools

import jax
import jax.numpy as jnp
import numpy as np
from jax import lax
from jax.experimental import pallas as pl
from jax.experimental.pallas import tpu as pltpu
from jax.sharding import Mesh
from jax.sharding import PartitionSpec as P


PREFILL = 320
X, ZO, ZI = 4, 8, 4
GX = ("x", "zo", "zi")
REP_GX = ("rep", "x", "zo", "zi")
LANES = 128
STEPS = (0, 1, 3, 2)
F32 = jnp.float32
BF16 = jnp.bfloat16


def shifted(value, axis, by):
    count = lax.axis_size(axis)
    return lax.ppermute(value, axis, [(i, (i + by) % count) for i in range(count)])


def exchanged(blocks, axes):
    return lax.all_to_all(blocks, axes, split_axis=0, concat_axis=0, tiled=True)


HBM = pl.BlockSpec(memory_space=pl.ANY)


def pass_on(ins, outs):
    for copy in ins:
        copy.start()
    for arrive, leave in zip(ins, outs, strict=True):
        arrive.wait()
        leave.start()
    for copy in outs:
        copy.wait()


def copies_kernel(kinds_ref, tokens_ref, out_ref):
    count, half = tokens_ref.shape
    row = lax.broadcasted_iota(jnp.int32, (count, LANES), 0)
    kinds = jnp.zeros((count, LANES), F32)
    for k in range(count):
        kinds = jnp.where(row == k, kinds_ref[k].astype(F32), kinds)
    for k in range(ZO):
        out_ref[k, :, :half] = tokens_ref[...]
        out_ref[k, :, half:] = kinds.astype(BF16)


def token_copies(tokens, segment_ids):
    count, half = tokens.shape
    return pl.pallas_call(
        copies_kernel,
        in_specs=[pl.BlockSpec(memory_space=pltpu.SMEM), pl.BlockSpec(memory_space=pltpu.VMEM)],
        out_specs=pl.BlockSpec(memory_space=pltpu.VMEM),
        out_shape=jax.ShapeDtypeStruct((ZO, count, half + LANES), tokens.dtype),
        name="token_copies",
    )(segment_ids, tokens)


def cut_by_x_kernel(x_ref, rows_ref, *refs):
    *outs, held, in_sems, out_sems = refs
    rows = held.shape[2]
    at = [pl.multiple_of(lax.rem(x_ref[0] + by, X) * rows, LANES) for by in STEPS]
    pass_on(
        [
            pltpu.make_async_copy(rows_ref.at[:, pl.ds(at[k], rows)], held.at[k], in_sems.at[k])
            for k in range(X)
        ],
        [pltpu.make_async_copy(held.at[k], outs[k], out_sems.at[k]) for k in range(X)],
    )


def cut_by_x(down, x):
    features, rows = down.shape
    out = jax.ShapeDtypeStruct((features, rows // X), down.dtype)
    blocks = pl.pallas_call(
        cut_by_x_kernel,
        in_specs=[pl.BlockSpec(memory_space=pltpu.SMEM), HBM],
        out_specs=[HBM] * X,
        out_shape=[out] * X,
        scratch_shapes=[
            pltpu.VMEM((X, *out.shape), down.dtype),
            pltpu.SemaphoreType.DMA((X,)),
            pltpu.SemaphoreType.DMA((X,)),
        ],
        name="cut_by_x",
    )(x, down)
    return list(blocks)


def split_kernel(gy_ref, gate_ref, up_ref, own_ref, other_ref, held, in_sems, out_sems):
    half = own_ref.shape[2]
    gy = gy_ref[0]
    ins, outs = [], []
    for k, ref in enumerate((gate_ref, up_ref)):
        for j, (out, which) in enumerate(((other_ref, 1 - gy), (own_ref, gy))):
            slot = 2 * k + j
            columns = pl.ds(pl.multiple_of(which * half, LANES), half)
            ins.append(pltpu.make_async_copy(ref.at[:, columns], held.at[slot], in_sems.at[slot]))
            outs.append(pltpu.make_async_copy(held.at[slot], out.at[k], out_sems.at[slot]))
    pass_on(ins, outs)


def split_rows(gate, up, gy):
    columns, both = gate.shape
    out = jax.ShapeDtypeStruct((2, columns, both // 2), gate.dtype)
    own, other = pl.pallas_call(
        split_kernel,
        in_specs=[pl.BlockSpec(memory_space=pltpu.SMEM), HBM, HBM],
        out_specs=[HBM, HBM],
        out_shape=[out, out],
        scratch_shapes=[
            pltpu.VMEM((4, columns, both // 2), gate.dtype),
            pltpu.SemaphoreType.DMA((4,)),
            pltpu.SemaphoreType.DMA((4,)),
        ],
        name="split_rows",
    )(gy, gate, up)
    return own.reshape(2 * columns, -1), other.reshape(2 * columns, -1)


def cut_by_zi_kernel(depth, x_ref, gy_ref, *refs):
    *rows_refs, out_ref = refs
    for by, rows_ref in zip(STEPS, rows_refs, strict=True):
        position = lax.rem(x_ref[0] + 2 * X - by - gy_ref[0] * (X // 2), X)
        for zi in range(ZI):
            pieces = [rows_ref[:, (zo * ZI + zi) * depth : (zo * ZI + zi + 1) * depth] for zo in range(ZO)]
            out_ref[zi, position] = jnp.concatenate(pieces, axis=1)


def cut_by_zi(blocks, x, gy):
    features, rows = blocks[0].shape
    depth = rows // (ZO * ZI)
    scalar = pl.BlockSpec(memory_space=pltpu.SMEM)
    whole = pl.BlockSpec(memory_space=pltpu.VMEM)
    return pl.pallas_call(
        functools.partial(cut_by_zi_kernel, depth),
        in_specs=[scalar, scalar] + [whole] * X,
        out_specs=whole,
        out_shape=jax.ShapeDtypeStruct((ZI, X, features, ZO * depth), blocks[0].dtype),
        name="cut_by_zi",
    )(x, gy, *blocks)


def place_kernel(x_ref, *refs):
    *kinds_refs, within_ref, within_row_ref, slot_ref, place_ref = refs
    chunk, count = within_ref.shape[0], slot_ref.shape[1]
    starts = [(lax.rem(x_ref[0] + X - by, X) * chunk).astype(F32) for by in STEPS]
    lane = lax.broadcasted_iota(jnp.int32, (1, count), 1)
    order_row = within_row_ref[...] + starts[0]
    for k in range(1, X):
        order_row = jnp.where(lane < k * chunk, order_row, within_row_ref[...] + starts[k])
    kinds = jnp.concatenate([ref[...] for ref in kinds_refs], 0)
    order = jnp.concatenate([within_ref[...] + start for start in starts], 0)
    earlier = (order_row < order[:, :1]).astype(BF16)
    decode_before = jnp.dot(earlier, kinds, preferred_element_type=F32)
    target = jnp.where(kinds.astype(F32) > 0.5, PREFILL + decode_before, order - decode_before)
    place_ref[...] = (target[:, :1] == slot_ref[...]).astype(BF16)


def placement(chunks, half, x, own_tokens):
    count = sum(chunk.shape[0] for chunk in chunks)
    chunk = count // X
    slot = np.arange(count, dtype=np.float32).reshape(X, ZO, ZI, own_tokens).transpose(0, 2, 1, 3)
    within = slot[0].reshape(chunk)
    kinds = [pl.BlockSpec((piece.shape[0], LANES), lambda i: (0, half // LANES)) for piece in chunks]
    row = pl.BlockSpec((1, count), lambda i: (0, 0))
    return pl.pallas_call(
        place_kernel,
        grid=(1,),
        in_specs=[pl.BlockSpec(memory_space=pltpu.SMEM)]
        + kinds
        + [pl.BlockSpec((chunk, LANES), lambda i: (0, 0)), row, row],
        out_specs=pl.BlockSpec((count, count), lambda i: (0, 0)),
        out_shape=jax.ShapeDtypeStruct((count, count), BF16),
        name="placement",
    )(
        x,
        *chunks,
        np.broadcast_to(within[:, None], (chunk, LANES)).copy(),
        np.tile(within, X).reshape(1, count),
        slot.reshape(1, count),
    )


def values_kernel(*refs):
    *chunk_refs, own_rows_ref, other_rows_ref, own_ref, other_ref = refs
    step = pl.program_id(0)
    columns = own_rows_ref.shape[0]
    chunks = jnp.concatenate([ref[...] for ref in chunk_refs], 0)
    rows = jnp.concatenate([own_rows_ref[...], other_rows_ref[...]], 0)
    term = lax.dot_general(rows, chunks, (((1,), (1,)), ((), ())), preferred_element_type=F32)

    @pl.when(step == 0)
    def _():
        own_ref[...] = term[:columns]
        other_ref[...] = term[columns:]

    @pl.when(step > 0)
    def _():
        own_ref[...] += term[:columns]
        other_ref[...] += term[columns:]


def values(chunks, own_rows, other_rows, steps=2):
    columns, half = own_rows.shape
    count = sum(chunk.shape[0] for chunk in chunks)
    depth = half // steps
    out = jax.ShapeDtypeStruct((columns, count), F32)
    rows = pl.BlockSpec((columns, depth), lambda i: (0, i))
    out_spec = pl.BlockSpec(out.shape, lambda i: (0, 0))
    return pl.pallas_call(
        values_kernel,
        grid=(steps,),
        in_specs=[pl.BlockSpec((chunk.shape[0], depth), lambda i: (0, i)) for chunk in chunks] + [rows, rows],
        out_specs=[out_spec, out_spec],
        out_shape=[out, out],
        name="values",
    )(*chunks, own_rows, other_rows)


def hidden_kernel(own_ref, other_ref, place_ref, out_ref):
    value = own_ref[...] + other_ref[...]
    width = value.shape[0] // 2
    gate_value, up_value = value[:width], value[width:]
    hidden = (gate_value / (1 + jnp.exp(-gate_value)) * up_value).astype(BF16)
    out_ref[...] = jnp.dot(hidden, place_ref[...], preferred_element_type=F32).astype(BF16)


def placed_hidden(own_value, other_value, place):
    return pl.pallas_call(
        hidden_kernel,
        out_shape=jax.ShapeDtypeStruct((own_value.shape[0] // 2, place.shape[1]), BF16),
        name="placed_hidden",
    )(own_value, other_value, place)


def block(tokens, segment_ids, gate_weight, up_weight, down_weight):
    x, gy = lax.axis_index("x"), lax.axis_index("gy")
    own_tokens, half = tokens.shape
    copies = token_copies(tokens, segment_ids)
    strided = exchanged(copies, "zo").reshape(ZO * own_tokens, -1)

    x_at, gy_at = x.reshape(1), gy.reshape(1)
    blocks = cut_by_x(down_weight[0].T, x_at)
    for k in range(1, X):
        blocks[k] = shifted(blocks[k], "x", STEPS[k])
    own_rows, other_rows = split_rows(gate_weight[:, 0].T, up_weight[:, 0].T, gy_at)
    other_rows = shifted(other_rows, "gy", 1)
    other_rows, *blocks = lax.optimization_barrier((other_rows, *blocks))
    group = cut_by_zi(blocks, x_at, gy_at)

    column = lax.all_gather(strided, "zi", axis=0, tiled=True)
    upper, lower = jnp.split(column, 2, axis=0)

    def passed(piece, by):
        return shifted(piece, "x", by)

    before_upper, after_lower = passed(upper, 1), passed(lower, 3)
    before_lower, after_upper = passed(lower, 1), passed(upper, 3)
    across_upper, across_lower = passed(before_upper, 1), passed(after_lower, 3)
    chunks = [column, before_upper, before_lower, after_upper, after_lower, across_upper, across_lower]

    group = exchanged(group, "zi")

    own_value, other_value = values(chunks, own_rows, other_rows)
    other_value = shifted(other_value, "gy", 1)
    place = placement(chunks, half, x_at, own_tokens)
    placed = placed_hidden(own_value, other_value, place)

    gathered = lax.all_gather(placed, "zo", axis=0, tiled=True)

    depth = group.shape[3]
    partial = lax.dot_general(
        gathered, group.reshape(-1, depth), (((0,), (1,)), ((), ())), preferred_element_type=F32
    )
    width = partial.shape[1] // (2 * ZI)

    def half_of(which):
        return jnp.concatenate(
            [partial[:, (2 * k + which) * width : (2 * k + which + 1) * width] for k in range(ZI)], 1
        )

    other_half = shifted(half_of(1).astype(BF16), "gy", 1)
    summed = (half_of(0) + other_half).astype(BF16)
    slots = summed.shape[0]
    arrived = exchanged(summed.reshape(X * ZI, slots // (X * ZI), -1), ("x", "zi"))
    reduced = jnp.sum(arrived.astype(F32), axis=0).astype(BF16)
    owned = exchanged(reduced.reshape(ZO, own_tokens, -1), "zo")
    owned = owned.reshape(ZO, own_tokens, ZI, X // 2, -1).transpose(1, 3, 0, 2, 4)
    return owned.reshape(own_tokens, half)


def solution(mesh):
    torus = Mesh(
        mesh.devices.reshape(mesh.shape["rep"], X, ZO, ZI, mesh.shape["gy"]),
        ("rep", "x", "zo", "zi", "gy"),
    )
    placed = (P(REP_GX, "gy"), P(REP_GX), P(None, "gy", GX), P(None, "gy", GX), P("gy", None, GX))
    return jax.shard_map(block, mesh=torus, in_specs=placed, out_specs=P(REP_GX, "gy"), check_vma=False)
```

```python
import functools

import jax
import jax.numpy as jnp
import numpy as np
from jax import lax
from jax.experimental import pallas as pl
from jax.experimental.pallas import tpu as pltpu
from jax.sharding import Mesh
from jax.sharding import PartitionSpec as P


PREFILL = 320
X, ZO, ZI = 4, 8, 4
GX = ("x", "zo", "zi")
REP_GX = ("rep", "x", "zo", "zi")
LANES = 128
STEPS = (0, 1, 3, 2)
F32 = jnp.float32
BF16 = jnp.bfloat16


def shifted(value, axis, by):
    count = lax.axis_size(axis)
    return lax.ppermute(value, axis, [(i, (i + by) % count) for i in range(count)])


def exchanged(blocks, axes):
    return lax.all_to_all(blocks, axes, split_axis=0, concat_axis=0, tiled=True)


HBM = pl.BlockSpec(memory_space=pl.ANY)


def pass_on(ins, outs):
    for copy in ins:
        copy.start()
    for arrive, leave in zip(ins, outs, strict=True):
        arrive.wait()
        leave.start()
    for copy in outs:
        copy.wait()


def copies_kernel(kinds_ref, tokens_ref, out_ref):
    count, half = tokens_ref.shape
    row = lax.broadcasted_iota(jnp.int32, (count, LANES), 0)
    kinds = jnp.zeros((count, LANES), F32)
    for k in range(count):
        kinds = jnp.where(row == k, kinds_ref[k].astype(F32), kinds)
    for k in range(ZO):
        out_ref[k, :, :half] = tokens_ref[...]
        out_ref[k, :, half:] = kinds.astype(BF16)


def token_copies(tokens, segment_ids):
    count, half = tokens.shape
    return pl.pallas_call(
        copies_kernel,
        in_specs=[pl.BlockSpec(memory_space=pltpu.SMEM), pl.BlockSpec(memory_space=pltpu.VMEM)],
        out_specs=pl.BlockSpec(memory_space=pltpu.VMEM),
        out_shape=jax.ShapeDtypeStruct((ZO, count, half + LANES), tokens.dtype),
        name="token_copies",
    )(segment_ids, tokens)


def cut_by_x_kernel(x_ref, rows_ref, *refs):
    *outs, held, in_sems, out_sems = refs
    rows = held.shape[2]
    at = [pl.multiple_of(lax.rem(x_ref[0] + by, X) * rows, LANES) for by in STEPS]
    pass_on(
        [
            pltpu.make_async_copy(rows_ref.at[:, pl.ds(at[k], rows)], held.at[k], in_sems.at[k])
            for k in range(X)
        ],
        [pltpu.make_async_copy(held.at[k], outs[k], out_sems.at[k]) for k in range(X)],
    )


def cut_by_x(down, x):
    features, rows = down.shape
    out = jax.ShapeDtypeStruct((features, rows // X), down.dtype)
    blocks = pl.pallas_call(
        cut_by_x_kernel,
        in_specs=[pl.BlockSpec(memory_space=pltpu.SMEM), HBM],
        out_specs=[HBM] * X,
        out_shape=[out] * X,
        scratch_shapes=[
            pltpu.VMEM((X, *out.shape), down.dtype),
            pltpu.SemaphoreType.DMA((X,)),
            pltpu.SemaphoreType.DMA((X,)),
        ],
        name="cut_by_x",
    )(x, down)
    return list(blocks)


def split_kernel(gy_ref, gate_ref, up_ref, own_ref, other_ref, held, in_sems, out_sems):
    half = own_ref.shape[2]
    gy = gy_ref[0]
    ins, outs = [], []
    for k, ref in enumerate((gate_ref, up_ref)):
        for j, (out, which) in enumerate(((other_ref, 1 - gy), (own_ref, gy))):
            slot = 2 * k + j
            columns = pl.ds(pl.multiple_of(which * half, LANES), half)
            ins.append(pltpu.make_async_copy(ref.at[:, columns], held.at[slot], in_sems.at[slot]))
            outs.append(pltpu.make_async_copy(held.at[slot], out.at[k], out_sems.at[slot]))
    pass_on(ins, outs)


def split_rows(gate, up, gy):
    columns, both = gate.shape
    out = jax.ShapeDtypeStruct((2, columns, both // 2), gate.dtype)
    own, other = pl.pallas_call(
        split_kernel,
        in_specs=[pl.BlockSpec(memory_space=pltpu.SMEM), HBM, HBM],
        out_specs=[HBM, HBM],
        out_shape=[out, out],
        scratch_shapes=[
            pltpu.VMEM((4, columns, both // 2), gate.dtype),
            pltpu.SemaphoreType.DMA((4,)),
            pltpu.SemaphoreType.DMA((4,)),
        ],
        name="split_rows",
    )(gy, gate, up)
    return own.reshape(2 * columns, -1), other.reshape(2 * columns, -1)


def cut_by_zi_kernel(depth, x_ref, gy_ref, *refs):
    *rows_refs, out_ref = refs
    for by, rows_ref in zip(STEPS, rows_refs, strict=True):
        position = lax.rem(x_ref[0] + 2 * X - by - gy_ref[0] * (X // 2), X)
        for zi in range(ZI):
            pieces = [rows_ref[:, (zo * ZI + zi) * depth : (zo * ZI + zi + 1) * depth] for zo in range(ZO)]
            out_ref[zi, position] = jnp.concatenate(pieces, axis=1)


def cut_by_zi(blocks, x, gy):
    features, rows = blocks[0].shape
    depth = rows // (ZO * ZI)
    scalar = pl.BlockSpec(memory_space=pltpu.SMEM)
    whole = pl.BlockSpec(memory_space=pltpu.VMEM)
    return pl.pallas_call(
        functools.partial(cut_by_zi_kernel, depth),
        in_specs=[scalar, scalar] + [whole] * X,
        out_specs=whole,
        out_shape=jax.ShapeDtypeStruct((ZI, X, features, ZO * depth), blocks[0].dtype),
        name="cut_by_zi",
    )(x, gy, *blocks)


def place_kernel(x_ref, *refs):
    *kinds_refs, within_ref, within_row_ref, slot_ref, place_ref = refs
    chunk, count = within_ref.shape[0], slot_ref.shape[1]
    starts = [(lax.rem(x_ref[0] + X - by, X) * chunk).astype(F32) for by in STEPS]
    lane = lax.broadcasted_iota(jnp.int32, (1, count), 1)
    order_row = within_row_ref[...] + starts[0]
    for k in range(1, X):
        order_row = jnp.where(lane < k * chunk, order_row, within_row_ref[...] + starts[k])
    kinds = jnp.concatenate([ref[...] for ref in kinds_refs], 0)
    order = jnp.concatenate([within_ref[...] + start for start in starts], 0)
    earlier = (order_row < order[:, :1]).astype(BF16)
    decode_before = jnp.dot(earlier, kinds, preferred_element_type=F32)
    target = jnp.where(kinds.astype(F32) > 0.5, PREFILL + decode_before, order - decode_before)
    place_ref[...] = (target[:, :1] == slot_ref[...]).astype(BF16)


def placement(chunks, half, x, own_tokens):
    count = sum(chunk.shape[0] for chunk in chunks)
    chunk = count // X
    slot = np.arange(count, dtype=np.float32).reshape(X, ZO, ZI, own_tokens).transpose(0, 2, 1, 3)
    within = slot[0].reshape(chunk)
    kinds = [pl.BlockSpec((piece.shape[0], LANES), lambda i: (0, half // LANES)) for piece in chunks]
    row = pl.BlockSpec((1, count), lambda i: (0, 0))
    return pl.pallas_call(
        place_kernel,
        grid=(1,),
        in_specs=[pl.BlockSpec(memory_space=pltpu.SMEM)]
        + kinds
        + [pl.BlockSpec((chunk, LANES), lambda i: (0, 0)), row, row],
        out_specs=pl.BlockSpec((count, count), lambda i: (0, 0)),
        out_shape=jax.ShapeDtypeStruct((count, count), BF16),
        name="placement",
    )(
        x,
        *chunks,
        np.broadcast_to(within[:, None], (chunk, LANES)).copy(),
        np.tile(within, X).reshape(1, count),
        slot.reshape(1, count),
    )


def values_kernel(*refs):
    *chunk_refs, own_rows_ref, other_rows_ref, own_ref, other_ref = refs
    step = pl.program_id(0)
    columns = own_rows_ref.shape[0]
    chunks = jnp.concatenate([ref[...] for ref in chunk_refs], 0)
    rows = jnp.concatenate([own_rows_ref[...], other_rows_ref[...]], 0)
    term = lax.dot_general(rows, chunks, (((1,), (1,)), ((), ())), preferred_element_type=F32)

    @pl.when(step == 0)
    def _():
        own_ref[...] = term[:columns]
        other_ref[...] = term[columns:]

    @pl.when(step > 0)
    def _():
        own_ref[...] += term[:columns]
        other_ref[...] += term[columns:]


def values(chunks, own_rows, other_rows, steps=2):
    columns, half = own_rows.shape
    count = sum(chunk.shape[0] for chunk in chunks)
    depth = half // steps
    out = jax.ShapeDtypeStruct((columns, count), F32)
    rows = pl.BlockSpec((columns, depth), lambda i: (0, i))
    out_spec = pl.BlockSpec(out.shape, lambda i: (0, 0))
    return pl.pallas_call(
        values_kernel,
        grid=(steps,),
        in_specs=[pl.BlockSpec((chunk.shape[0], depth), lambda i: (0, i)) for chunk in chunks] + [rows, rows],
        out_specs=[out_spec, out_spec],
        out_shape=[out, out],
        name="values",
    )(*chunks, own_rows, other_rows)


def placed_hidden(own_value, other_value, place):
    value = own_value + other_value
    gate_value, up_value = jnp.split(value, 2, axis=0)
    hidden = (gate_value / (1 + jnp.exp(-gate_value)) * up_value).astype(BF16)
    return jnp.dot(hidden, place, preferred_element_type=F32).astype(BF16)


def block(tokens, segment_ids, gate_weight, up_weight, down_weight):
    x, gy = lax.axis_index("x"), lax.axis_index("gy")
    own_tokens, half = tokens.shape
    copies = token_copies(tokens, segment_ids)
    strided = exchanged(copies, "zo").reshape(ZO * own_tokens, -1)

    x_at, gy_at = x.reshape(1), gy.reshape(1)
    blocks = cut_by_x(down_weight[0].T, x_at)
    for k in range(1, X):
        blocks[k] = shifted(blocks[k], "x", STEPS[k])
    own_rows, other_rows = split_rows(gate_weight[:, 0].T, up_weight[:, 0].T, gy_at)
    other_rows = shifted(other_rows, "gy", 1)
    other_rows, *blocks = lax.optimization_barrier((other_rows, *blocks))
    group = cut_by_zi(blocks, x_at, gy_at)

    column = lax.all_gather(strided, "zi", axis=0, tiled=True)
    upper, lower = jnp.split(column, 2, axis=0)

    def passed(piece, by):
        return shifted(piece, "x", by)

    before_upper, after_lower = passed(upper, 1), passed(lower, 3)
    before_lower, after_upper = passed(lower, 1), passed(upper, 3)
    across_upper, across_lower = passed(before_upper, 1), passed(after_lower, 3)
    chunks = [column, before_upper, before_lower, after_upper, after_lower, across_upper, across_lower]

    group = exchanged(group, "zi")

    own_value, other_value = values(chunks, own_rows, other_rows)
    other_value = shifted(other_value, "gy", 1)
    place = placement(chunks, half, x_at, own_tokens)
    placed = placed_hidden(own_value, other_value, place)

    gathered = lax.all_gather(placed, "zo", axis=0, tiled=True)

    depth = group.shape[3]
    partial = lax.dot_general(
        gathered, group.reshape(-1, depth), (((0,), (1,)), ((), ())), preferred_element_type=F32
    )
    width = partial.shape[1] // (2 * ZI)

    def half_of(which):
        return jnp.concatenate(
            [partial[:, (2 * k + which) * width : (2 * k + which + 1) * width] for k in range(ZI)], 1
        )

    other_half = shifted(half_of(1).astype(BF16), "gy", 1)
    summed = (half_of(0) + other_half).astype(BF16)
    slots = summed.shape[0]
    arrived = exchanged(summed.reshape(X * ZI, slots // (X * ZI), -1), ("x", "zi"))
    reduced = jnp.sum(arrived.astype(F32), axis=0).astype(BF16)
    owned = exchanged(reduced.reshape(ZO, own_tokens, -1), "zo")
    owned = owned.reshape(ZO, own_tokens, ZI, X // 2, -1).transpose(1, 3, 0, 2, 4)
    return owned.reshape(own_tokens, half)


def solution(mesh):
    torus = Mesh(
        mesh.devices.reshape(mesh.shape["rep"], X, ZO, ZI, mesh.shape["gy"]),
        ("rep", "x", "zo", "zi", "gy"),
    )
    placed = (P(REP_GX, "gy"), P(REP_GX), P(None, "gy", GX), P(None, "gy", GX), P("gy", None, GX))
    return jax.shard_map(block, mesh=torus, in_specs=placed, out_specs=P(REP_GX, "gy"), check_vma=False)
```

```python
import functools

import jax
import jax.numpy as jnp
import numpy as np
from jax import lax
from jax.experimental import pallas as pl
from jax.experimental.pallas import tpu as pltpu
from jax.sharding import Mesh
from jax.sharding import PartitionSpec as P


PREFILL = 320
X, ZO, ZI = 4, 8, 4
GX = ("x", "zo", "zi")
REP_GX = ("rep", "x", "zo", "zi")
LANES = 128
STEPS = (0, 1, 3, 2)
F32 = jnp.float32
BF16 = jnp.bfloat16


def shifted(value, axis, by):
    count = lax.axis_size(axis)
    return lax.ppermute(value, axis, [(i, (i + by) % count) for i in range(count)])


def exchanged(blocks, axes):
    return lax.all_to_all(blocks, axes, split_axis=0, concat_axis=0, tiled=True)


HBM = pl.BlockSpec(memory_space=pl.ANY)


def pass_on(ins, outs):
    for copy in ins:
        copy.start()
    for arrive, leave in zip(ins, outs, strict=True):
        arrive.wait()
        leave.start()
    for copy in outs:
        copy.wait()


def copies_kernel(kinds_ref, tokens_ref, out_ref):
    count, half = tokens_ref.shape
    row = lax.broadcasted_iota(jnp.int32, (count, LANES), 0)
    kinds = jnp.zeros((count, LANES), F32)
    for k in range(count):
        kinds = jnp.where(row == k, kinds_ref[k].astype(F32), kinds)
    for k in range(ZO):
        out_ref[k, :, :half] = tokens_ref[...]
        out_ref[k, :, half:] = kinds.astype(BF16)


def token_copies(tokens, segment_ids):
    count, half = tokens.shape
    return pl.pallas_call(
        copies_kernel,
        in_specs=[pl.BlockSpec(memory_space=pltpu.SMEM), pl.BlockSpec(memory_space=pltpu.VMEM)],
        out_specs=pl.BlockSpec(memory_space=pltpu.VMEM),
        out_shape=jax.ShapeDtypeStruct((ZO, count, half + LANES), tokens.dtype),
        name="token_copies",
    )(segment_ids, tokens)


def cut_by_x_kernel(x_ref, rows_ref, *refs):
    *outs, held, in_sems, out_sems = refs
    rows = held.shape[2]
    at = [pl.multiple_of(lax.rem(x_ref[0] + by, X) * rows, LANES) for by in STEPS]
    pass_on(
        [
            pltpu.make_async_copy(rows_ref.at[:, pl.ds(at[k], rows)], held.at[k], in_sems.at[k])
            for k in range(X)
        ],
        [pltpu.make_async_copy(held.at[k], outs[k], out_sems.at[k]) for k in range(X)],
    )


def cut_by_x(down, x):
    features, rows = down.shape
    out = jax.ShapeDtypeStruct((features, rows // X), down.dtype)
    blocks = pl.pallas_call(
        cut_by_x_kernel,
        in_specs=[pl.BlockSpec(memory_space=pltpu.SMEM), HBM],
        out_specs=[HBM] * X,
        out_shape=[out] * X,
        scratch_shapes=[
            pltpu.VMEM((X, *out.shape), down.dtype),
            pltpu.SemaphoreType.DMA((X,)),
            pltpu.SemaphoreType.DMA((X,)),
        ],
        name="cut_by_x",
    )(x, down)
    return list(blocks)


def split_kernel(gy_ref, gate_ref, up_ref, own_ref, other_ref, held, in_sems, out_sems):
    half = own_ref.shape[2]
    gy = gy_ref[0]
    ins, outs = [], []
    for k, ref in enumerate((gate_ref, up_ref)):
        for j, (out, which) in enumerate(((other_ref, 1 - gy), (own_ref, gy))):
            slot = 2 * k + j
            columns = pl.ds(pl.multiple_of(which * half, LANES), half)
            ins.append(pltpu.make_async_copy(ref.at[:, columns], held.at[slot], in_sems.at[slot]))
            outs.append(pltpu.make_async_copy(held.at[slot], out.at[k], out_sems.at[slot]))
    pass_on(ins, outs)


def split_rows(gate, up, gy):
    columns, both = gate.shape
    out = jax.ShapeDtypeStruct((2, columns, both // 2), gate.dtype)
    own, other = pl.pallas_call(
        split_kernel,
        in_specs=[pl.BlockSpec(memory_space=pltpu.SMEM), HBM, HBM],
        out_specs=[HBM, HBM],
        out_shape=[out, out],
        scratch_shapes=[
            pltpu.VMEM((4, columns, both // 2), gate.dtype),
            pltpu.SemaphoreType.DMA((4,)),
            pltpu.SemaphoreType.DMA((4,)),
        ],
        name="split_rows",
    )(gy, gate, up)
    return own.reshape(2 * columns, -1), other.reshape(2 * columns, -1)


def cut_by_zi_kernel(depth, x_ref, gy_ref, *refs):
    *rows_refs, out_ref = refs
    for by, rows_ref in zip(STEPS, rows_refs, strict=True):
        position = lax.rem(x_ref[0] + 2 * X - by - gy_ref[0] * (X // 2), X)
        for zi in range(ZI):
            pieces = [rows_ref[:, (zo * ZI + zi) * depth : (zo * ZI + zi + 1) * depth] for zo in range(ZO)]
            out_ref[zi, position] = jnp.concatenate(pieces, axis=1)


def cut_by_zi(blocks, x, gy):
    features, rows = blocks[0].shape
    depth = rows // (ZO * ZI)
    scalar = pl.BlockSpec(memory_space=pltpu.SMEM)
    whole = pl.BlockSpec(memory_space=pltpu.VMEM)
    return pl.pallas_call(
        functools.partial(cut_by_zi_kernel, depth),
        in_specs=[scalar, scalar] + [whole] * X,
        out_specs=whole,
        out_shape=jax.ShapeDtypeStruct((ZI, X, features, ZO * depth), blocks[0].dtype),
        name="cut_by_zi",
    )(x, gy, *blocks)


def place_kernel(x_ref, *refs):
    *kinds_refs, within_ref, within_row_ref, slot_ref, place_ref = refs
    chunk, count = within_ref.shape[0], slot_ref.shape[1]
    starts = [(lax.rem(x_ref[0] + X - by, X) * chunk).astype(F32) for by in STEPS]
    lane = lax.broadcasted_iota(jnp.int32, (1, count), 1)
    order_row = within_row_ref[...] + starts[0]
    for k in range(1, X):
        order_row = jnp.where(lane < k * chunk, order_row, within_row_ref[...] + starts[k])
    kinds = jnp.concatenate([ref[...] for ref in kinds_refs], 0)
    order = jnp.concatenate([within_ref[...] + start for start in starts], 0)
    earlier = (order_row < order[:, :1]).astype(BF16)
    decode_before = jnp.dot(earlier, kinds, preferred_element_type=F32)
    target = jnp.where(kinds.astype(F32) > 0.5, PREFILL + decode_before, order - decode_before)
    place_ref[...] = (target[:, :1] == slot_ref[...]).astype(BF16)


def placement(chunks, half, x, own_tokens):
    count = sum(chunk.shape[0] for chunk in chunks)
    chunk = count // X
    slot = np.arange(count, dtype=np.float32).reshape(X, ZO, ZI, own_tokens).transpose(0, 2, 1, 3)
    within = slot[0].reshape(chunk)
    kinds = [pl.BlockSpec((piece.shape[0], LANES), lambda i: (0, half // LANES)) for piece in chunks]
    row = pl.BlockSpec((1, count), lambda i: (0, 0))
    return pl.pallas_call(
        place_kernel,
        grid=(1,),
        in_specs=[pl.BlockSpec(memory_space=pltpu.SMEM)]
        + kinds
        + [pl.BlockSpec((chunk, LANES), lambda i: (0, 0)), row, row],
        out_specs=pl.BlockSpec((count, count), lambda i: (0, 0)),
        out_shape=jax.ShapeDtypeStruct((count, count), BF16),
        name="placement",
    )(
        x,
        *chunks,
        np.broadcast_to(within[:, None], (chunk, LANES)).copy(),
        np.tile(within, X).reshape(1, count),
        slot.reshape(1, count),
    )


def placed_hidden(own_value, other_value, place):
    value = own_value + other_value
    gate_value, up_value = jnp.split(value, 2, axis=0)
    hidden = (gate_value / (1 + jnp.exp(-gate_value)) * up_value).astype(BF16)
    return jnp.dot(hidden, place, preferred_element_type=F32).astype(BF16)


def block(tokens, segment_ids, gate_weight, up_weight, down_weight):
    x, gy = lax.axis_index("x"), lax.axis_index("gy")
    own_tokens, half = tokens.shape
    copies = token_copies(tokens, segment_ids)
    strided = exchanged(copies, "zo").reshape(ZO * own_tokens, -1)

    x_at, gy_at = x.reshape(1), gy.reshape(1)
    blocks = cut_by_x(down_weight[0].T, x_at)
    for k in range(1, X):
        blocks[k] = shifted(blocks[k], "x", STEPS[k])
    own_rows, other_rows = split_rows(gate_weight[:, 0].T, up_weight[:, 0].T, gy_at)
    other_rows = shifted(other_rows, "gy", 1)
    other_rows, *blocks = lax.optimization_barrier((other_rows, *blocks))
    group = cut_by_zi(blocks, x_at, gy_at)

    column = lax.all_gather(strided, "zi", axis=0, tiled=True)
    upper, lower = jnp.split(column, 2, axis=0)

    def passed(piece, by):
        return shifted(piece, "x", by)

    before_upper, after_lower = passed(upper, 1), passed(lower, 3)
    before_lower, after_upper = passed(lower, 1), passed(upper, 3)
    across_upper, across_lower = passed(before_upper, 1), passed(after_lower, 3)
    chunks = [column, before_upper, before_lower, after_upper, after_lower, across_upper, across_lower]

    group = exchanged(group, "zi")

    tokens_all = jnp.concatenate([chunk[:, :half] for chunk in chunks], 0)

    def values(rows):
        return lax.dot_general(rows, tokens_all, (((1,), (1,)), ((), ())), preferred_element_type=F32)

    other_value, own_value = values(other_rows), values(own_rows)
    other_value = shifted(other_value, "gy", 1)
    place = placement(chunks, half, x_at, own_tokens)
    placed = placed_hidden(own_value, other_value, place)

    gathered = lax.all_gather(placed, "zo", axis=0, tiled=True)

    depth = group.shape[3]
    partial = lax.dot_general(
        gathered, group.reshape(-1, depth), (((0,), (1,)), ((), ())), preferred_element_type=F32
    )
    width = partial.shape[1] // (2 * ZI)

    def half_of(which):
        return jnp.concatenate(
            [partial[:, (2 * k + which) * width : (2 * k + which + 1) * width] for k in range(ZI)], 1
        )

    other_half = shifted(half_of(1).astype(BF16), "gy", 1)
    summed = (half_of(0) + other_half).astype(BF16)
    slots = summed.shape[0]
    arrived = exchanged(summed.reshape(X * ZI, slots // (X * ZI), -1), ("x", "zi"))
    reduced = jnp.sum(arrived.astype(F32), axis=0).astype(BF16)
    owned = exchanged(reduced.reshape(ZO, own_tokens, -1), "zo")
    owned = owned.reshape(ZO, own_tokens, ZI, X // 2, -1).transpose(1, 3, 0, 2, 4)
    return owned.reshape(own_tokens, half)


def solution(mesh):
    torus = Mesh(
        mesh.devices.reshape(mesh.shape["rep"], X, ZO, ZI, mesh.shape["gy"]),
        ("rep", "x", "zo", "zi", "gy"),
    )
    placed = (P(REP_GX, "gy"), P(REP_GX), P(None, "gy", GX), P(None, "gy", GX), P("gy", None, GX))
    return jax.shard_map(block, mesh=torus, in_specs=placed, out_specs=P(REP_GX, "gy"), check_vma=False)
```

```python
import functools

import jax
import jax.numpy as jnp
import numpy as np
from jax import lax
from jax.experimental import pallas as pl
from jax.experimental.pallas import tpu as pltpu
from jax.sharding import Mesh
from jax.sharding import PartitionSpec as P


PREFILL = 320
X, ZO, ZI = 4, 8, 4
GX = ("x", "zo", "zi")
REP_GX = ("rep", "x", "zo", "zi")
LANES = 128
STEPS = (0, 1, 3, 2)
F32 = jnp.float32
BF16 = jnp.bfloat16


def shifted(value, axis, by):
    count = lax.axis_size(axis)
    return lax.ppermute(value, axis, [(i, (i + by) % count) for i in range(count)])


def exchanged(blocks, axes):
    return lax.all_to_all(blocks, axes, split_axis=0, concat_axis=0, tiled=True)


HBM = pl.BlockSpec(memory_space=pl.ANY)


def pass_on(ins, outs):
    for copy in ins:
        copy.start()
    for arrive, leave in zip(ins, outs, strict=True):
        arrive.wait()
        leave.start()
    for copy in outs:
        copy.wait()


def copies_kernel(kinds_ref, tokens_ref, out_ref):
    count, half = tokens_ref.shape
    row = lax.broadcasted_iota(jnp.int32, (count, LANES), 0)
    kinds = jnp.zeros((count, LANES), F32)
    for k in range(count):
        kinds = jnp.where(row == k, kinds_ref[k].astype(F32), kinds)
    for k in range(ZO):
        out_ref[k, :, :half] = tokens_ref[...]
        out_ref[k, :, half:] = kinds.astype(BF16)


def token_copies(tokens, segment_ids):
    count, half = tokens.shape
    return pl.pallas_call(
        copies_kernel,
        in_specs=[pl.BlockSpec(memory_space=pltpu.SMEM), pl.BlockSpec(memory_space=pltpu.VMEM)],
        out_specs=pl.BlockSpec(memory_space=pltpu.VMEM),
        out_shape=jax.ShapeDtypeStruct((ZO, count, half + LANES), tokens.dtype),
        name="token_copies",
    )(segment_ids, tokens)


def cut_by_x_kernel(x_ref, rows_ref, *refs):
    *outs, held, in_sems, out_sems = refs
    rows = held.shape[2]
    at = [pl.multiple_of(lax.rem(x_ref[0] + by, X) * rows, LANES) for by in STEPS]
    pass_on(
        [
            pltpu.make_async_copy(rows_ref.at[:, pl.ds(at[k], rows)], held.at[k], in_sems.at[k])
            for k in range(X)
        ],
        [pltpu.make_async_copy(held.at[k], outs[k], out_sems.at[k]) for k in range(X)],
    )


def cut_by_x(down, x):
    features, rows = down.shape
    out = jax.ShapeDtypeStruct((features, rows // X), down.dtype)
    blocks = pl.pallas_call(
        cut_by_x_kernel,
        in_specs=[pl.BlockSpec(memory_space=pltpu.SMEM), HBM],
        out_specs=[HBM] * X,
        out_shape=[out] * X,
        scratch_shapes=[
            pltpu.VMEM((X, *out.shape), down.dtype),
            pltpu.SemaphoreType.DMA((X,)),
            pltpu.SemaphoreType.DMA((X,)),
        ],
        name="cut_by_x",
    )(x, down)
    return list(blocks)


def split_kernel(gy_ref, gate_ref, up_ref, own_ref, other_ref, held, in_sems, out_sems):
    half = own_ref.shape[2]
    gy = gy_ref[0]
    ins, outs = [], []
    for k, ref in enumerate((gate_ref, up_ref)):
        for j, (out, which) in enumerate(((other_ref, 1 - gy), (own_ref, gy))):
            slot = 2 * k + j
            columns = pl.ds(pl.multiple_of(which * half, LANES), half)
            ins.append(pltpu.make_async_copy(ref.at[:, columns], held.at[slot], in_sems.at[slot]))
            outs.append(pltpu.make_async_copy(held.at[slot], out.at[k], out_sems.at[slot]))
    pass_on(ins, outs)


def split_rows(gate, up, gy):
    columns, both = gate.shape
    out = jax.ShapeDtypeStruct((2, columns, both // 2), gate.dtype)
    own, other = pl.pallas_call(
        split_kernel,
        in_specs=[pl.BlockSpec(memory_space=pltpu.SMEM), HBM, HBM],
        out_specs=[HBM, HBM],
        out_shape=[out, out],
        scratch_shapes=[
            pltpu.VMEM((4, columns, both // 2), gate.dtype),
            pltpu.SemaphoreType.DMA((4,)),
            pltpu.SemaphoreType.DMA((4,)),
        ],
        name="split_rows",
    )(gy, gate, up)
    return own.reshape(2 * columns, -1), other.reshape(2 * columns, -1)


def cut_by_zi_kernel(depth, x_ref, gy_ref, *refs):
    *rows_refs, out_ref = refs
    for by, rows_ref in zip(STEPS, rows_refs, strict=True):
        position = lax.rem(x_ref[0] + 2 * X - by - gy_ref[0] * (X // 2), X)
        for zi in range(ZI):
            pieces = [rows_ref[:, (zo * ZI + zi) * depth : (zo * ZI + zi + 1) * depth] for zo in range(ZO)]
            out_ref[zi, position] = jnp.concatenate(pieces, axis=1)


def cut_by_zi(blocks, x, gy):
    features, rows = blocks[0].shape
    depth = rows // (ZO * ZI)
    scalar = pl.BlockSpec(memory_space=pltpu.SMEM)
    whole = pl.BlockSpec(memory_space=pltpu.VMEM)
    return pl.pallas_call(
        functools.partial(cut_by_zi_kernel, depth),
        in_specs=[scalar, scalar] + [whole] * X,
        out_specs=whole,
        out_shape=jax.ShapeDtypeStruct((ZI, X, features, ZO * depth), blocks[0].dtype),
        name="cut_by_zi",
    )(x, gy, *blocks)


def place_kernel(x_ref, *refs):
    *kinds_refs, within_ref, within_row_ref, slot_ref, place_ref = refs
    chunk, count = within_ref.shape[0], slot_ref.shape[1]
    starts = [(lax.rem(x_ref[0] + X - by, X) * chunk).astype(F32) for by in STEPS]
    lane = lax.broadcasted_iota(jnp.int32, (1, count), 1)
    order_row = within_row_ref[...] + starts[0]
    for k in range(1, X):
        order_row = jnp.where(lane < k * chunk, order_row, within_row_ref[...] + starts[k])
    kinds = jnp.concatenate([ref[...] for ref in kinds_refs], 0)
    order = jnp.concatenate([within_ref[...] + start for start in starts], 0)
    earlier = (order_row < order[:, :1]).astype(BF16)
    decode_before = jnp.dot(earlier, kinds, preferred_element_type=F32)
    target = jnp.where(kinds.astype(F32) > 0.5, PREFILL + decode_before, order - decode_before)
    place_ref[...] = (target[:, :1] == slot_ref[...]).astype(BF16)


def placement(chunks, half, x, own_tokens):
    count = sum(chunk.shape[0] for chunk in chunks)
    chunk = count // X
    slot = np.arange(count, dtype=np.float32).reshape(X, ZO, ZI, own_tokens).transpose(0, 2, 1, 3)
    within = slot[0].reshape(chunk)
    kinds = [pl.BlockSpec((piece.shape[0], LANES), lambda i: (0, half // LANES)) for piece in chunks]
    row = pl.BlockSpec((1, count), lambda i: (0, 0))
    return pl.pallas_call(
        place_kernel,
        grid=(1,),
        in_specs=[pl.BlockSpec(memory_space=pltpu.SMEM)]
        + kinds
        + [pl.BlockSpec((chunk, LANES), lambda i: (0, 0)), row, row],
        out_specs=pl.BlockSpec((count, count), lambda i: (0, 0)),
        out_shape=jax.ShapeDtypeStruct((count, count), BF16),
        name="placement",
    )(
        x,
        *chunks,
        np.broadcast_to(within[:, None], (chunk, LANES)).copy(),
        np.tile(within, X).reshape(1, count),
        slot.reshape(1, count),
    )


def placed_hidden(own_value, other_value, place):
    value = own_value + other_value
    gate_value, up_value = jnp.split(value, 2, axis=0)
    hidden = (gate_value / (1 + jnp.exp(-gate_value)) * up_value).astype(BF16)
    return jnp.dot(hidden, place, preferred_element_type=F32).astype(BF16)


def block(tokens, segment_ids, gate_weight, up_weight, down_weight):
    x, gy = lax.axis_index("x"), lax.axis_index("gy")
    own_tokens, half = tokens.shape
    copies = token_copies(tokens, segment_ids)
    strided = exchanged(copies, "zo").reshape(ZO * own_tokens, -1)

    x_at, gy_at = x.reshape(1), gy.reshape(1)
    blocks = cut_by_x(down_weight[0].T, x_at)
    for k in range(1, X):
        blocks[k] = shifted(blocks[k], "x", STEPS[k])
    own_rows, other_rows = split_rows(gate_weight[:, 0].T, up_weight[:, 0].T, gy_at)
    other_rows = shifted(other_rows, "gy", 1)
    other_rows, *blocks = lax.optimization_barrier((other_rows, *blocks))
    group = cut_by_zi(blocks, x_at, gy_at)

    column = lax.all_gather(strided, "zi", axis=0, tiled=True)
    upper, lower = jnp.split(column, 2, axis=0)

    def passed(piece, by):
        return shifted(piece, "x", by)

    before_upper, after_lower = passed(upper, 1), passed(lower, 3)
    before_lower, after_upper = passed(lower, 1), passed(upper, 3)
    across_upper, across_lower = passed(before_upper, 1), passed(after_lower, 3)
    chunks = [column, before_upper, before_lower, after_upper, after_lower, across_upper, across_lower]

    group = exchanged(group, "zi")

    rows = jnp.concatenate([own_rows, other_rows], 0)
    tokens_all = jnp.concatenate([chunk[:, :half] for chunk in chunks], 0)
    value = lax.dot_general(rows, tokens_all, (((1,), (1,)), ((), ())), preferred_element_type=F32)
    own_value, other_value = jnp.split(value, 2, axis=0)
    other_value = shifted(other_value.astype(BF16), "gy", 1)
    place = placement(chunks, half, x_at, own_tokens)
    placed = placed_hidden(own_value, other_value, place)

    gathered = lax.all_gather(placed, "zo", axis=0, tiled=True)

    depth = group.shape[3]
    partial = lax.dot_general(
        gathered, group.reshape(-1, depth), (((0,), (1,)), ((), ())), preferred_element_type=F32
    )
    width = partial.shape[1] // (2 * ZI)

    def half_of(which):
        return jnp.concatenate(
            [partial[:, (2 * k + which) * width : (2 * k + which + 1) * width] for k in range(ZI)], 1
        )

    other_half = shifted(half_of(1).astype(BF16), "gy", 1)
    summed = (half_of(0) + other_half).astype(BF16)
    slots = summed.shape[0]
    arrived = exchanged(summed.reshape(X * ZI, slots // (X * ZI), -1), ("x", "zi"))
    reduced = jnp.sum(arrived.astype(F32), axis=0).astype(BF16)
    owned = exchanged(reduced.reshape(ZO, own_tokens, -1), "zo")
    owned = owned.reshape(ZO, own_tokens, ZI, X // 2, -1).transpose(1, 3, 0, 2, 4)
    return owned.reshape(own_tokens, half)


def solution(mesh):
    torus = Mesh(
        mesh.devices.reshape(mesh.shape["rep"], X, ZO, ZI, mesh.shape["gy"]),
        ("rep", "x", "zo", "zi", "gy"),
    )
    placed = (P(REP_GX, "gy"), P(REP_GX), P(None, "gy", GX), P(None, "gy", GX), P("gy", None, GX))
    return jax.shard_map(block, mesh=torus, in_specs=placed, out_specs=P(REP_GX, "gy"), check_vma=False)
```
